128 devices in a mesh: dp: 8 (over y_lo, z), head: 16 (over x, y_hi, core).
Axes of the slice: x: 4, y: 4 (y_hi: 2, y_lo: 2; y = y_hi * 2 + y_lo), z: 4, core: 2. Of those that a mesh axis runs over, the one named last changes fastest.
Arguments:
- projected: bfloat16 [49152, 24576], P(('dp', 'head')), may hold values from -64 to 64, as said below
- weight_exp: int32 [49152], P(('dp', 'head')), may hold values from 0 to 3
- damp_exp: int32 [128], replicated, may hold values from 0 to 2
Outputs:
- whitening: float32 [128, 192, 192], P('head')
The draws below stay inside these ranges and needn't reach their ends.
Inputs may be any that keep to these rules, and one draw needn't show every extreme that they name: `projected`: real values.
All inputs are finite; a program needn't handle non-finite values.
Results may differ from the reference program's by a relative error of at most 0.0003.
Values may be sent and summed in bfloat16 or wider, within the bound.
A program may use at most 192 MiB of HBM per device.

```python
import math
import jax
import jax.numpy as jnp
from jax import lax

HEADS = 64
HD = 192
TOKENS = 49152
MATS = 128


def draw_projected(key, part):
    first, second = jax.random.split(jax.random.fold_in(key, 11))
    base = jax.random.normal(first, (TOKENS, 2 * HEADS, HD), jnp.float32)
    scales = jnp.exp(jax.random.uniform(second, (2 * HEADS, HD), jnp.float32, 0.0, math.log(8.0)))
    mixed = base + 0.6 * jnp.roll(base, 1, axis=2) - 0.4 * jnp.roll(base, 5, axis=2)
    return jnp.clip((mixed * scales).reshape(TOKENS, 2 * HEADS * HD) / 4.0, -64.0, 64.0).astype(jnp.bfloat16)


def place_ends(entries, own_key, smallest, largest):
    longest = entries.shape.index(max(entries.shape))
    spots = []
    for shift in (0, 1):
        where = [jax.random.randint(jax.random.fold_in(own_key, axis), (), 0, length) for axis, length in enumerate(entries.shape)]
        where[longest] = (where[longest] + shift) % entries.shape[longest]
        spots.append(tuple(where))
    return entries.at[spots[0]].set(smallest).at[spots[1]].set(largest)


def setup_inputs(seed: int = 0) -> dict:
    seeds = jax.random.split(jax.random.key(seed), 4)
    return {
        "projected": draw_projected(jax.random.fold_in(seeds[3], 71), 0),
        "weight_exp": place_ends(jax.random.randint(seeds[1], (TOKENS,), 0, 4), jax.random.fold_in(seeds[1], 1), 0, 3).astype(jnp.int32),
        "damp_exp": place_ends(jax.random.randint(seeds[2], (MATS,), 0, 3), jax.random.fold_in(seeds[2], 1), 0, 2).astype(jnp.int32),
    }


def reference(projected, weight_exp, damp_exp):
    mats = projected.shape[1] // HD
    weights = jnp.exp2(weight_exp.astype(jnp.float32)).astype(jnp.bfloat16)
    scaled = projected * weights[:, None]
    eye = jnp.eye(HD, dtype=jnp.float32)

    def single(index):
        start = (index * HD).astype(jnp.int32)
        left = lax.dynamic_slice_in_dim(projected, start, HD, 1)
        right = lax.dynamic_slice_in_dim(scaled, start, HD, 1)
        gram = jnp.dot(left.T.astype(jnp.float32), right.astype(jnp.float32), preferred_element_type=jnp.float32) / TOKENS
        gram = 0.5 * (gram + gram.T)
        level = jnp.trace(gram) / HD + 1e-06
        damping = jnp.exp2(-damp_exp[index].astype(jnp.float32)) * level
        lower = jnp.linalg.cholesky(gram + damping * eye)
        return jax.scipy.linalg.solve_triangular(lower, eye, lower=True)
    return lax.map(single, jnp.arange(mats, dtype=jnp.int32))
```

```python
import functools

import jax
import jax.numpy as jnp
from jax import lax
from jax.experimental import pallas as pl
from jax.experimental.pallas import tpu as pltpu
from jax.sharding import PartitionSpec as P

HD = 192
BLK = HD // 3
HIGH = lax.Precision.HIGHEST


def store_pair(rows, wide, out, at, after):
    weighted = rows * wide
    contract = (((0,), (0,)), ((), ()))
    width = 4 * BLK
    first = lax.dot_general(rows[:, :width], weighted[:, :width], contract, preferred_element_type=jnp.float32)
    second = lax.dot_general(rows[:, -width:], weighted[:, -width:], contract, preferred_element_type=jnp.float32)
    two = 2 * BLK
    lanes = lax.broadcasted_iota(jnp.int32, (BLK, two), 1)
    corner = pltpu.roll(first[two : two + BLK, two:], BLK, 1)
    out[at, :BLK, :] = jnp.where(lanes < BLK, first[:BLK, :two], corner)
    out[at, BLK:, :] = first[BLK:HD, :two]
    out[after, :two, :] = second[BLK : BLK + two, two:]
    corner = pltpu.roll(second[BLK:two, :two], BLK, 1)
    out[after, two:, :] = jnp.where(lanes < BLK, corner, second[HD:, two:])


def dot(a, b):
    return lax.dot_general(a, b, (((1,), (0,)), ((), ())), precision=HIGH, preferred_element_type=jnp.float32)


def dot_t(a, b):
    return lax.dot_general(a, b, (((1,), (1,)), ((), ())), precision=HIGH, preferred_element_type=jnp.float32)


def inverse_factors(blocks):
    lane = lax.broadcasted_iota(jnp.int32, (8, BLK), 1)
    sub = lax.broadcasted_iota(jnp.int32, (8, BLK), 0)
    sub1 = lax.broadcasted_iota(jnp.int32, (8, 1), 0)
    groups = BLK // 8
    held = [[block[8 * g : 8 * g + 8] for g in range(groups)] for block in blocks]
    for k in range(BLK):
        own, spot = divmod(k, 8)
        is_k = lane == k
        for parts in held:
            row = parts[own][spot : spot + 1, :]
            scale = 1.0 / row[:, k : k + 1]
            row = jnp.where(is_k[:1], 1.0, row) * scale
            for g in range(own, groups):
                part = parts[g]
                column = part[:, k : k + 1]
                if g == own:
                    if spot == 7:
                        continue
                    column = jnp.where(sub1 > spot, column, 0.0)
                    kept = jnp.where(is_k & (sub > spot), 0.0, part)
                else:
                    kept = jnp.where(is_k, 0.0, part)
                parts[g] = kept - column * row
    out = []
    for parts in held:
        rows = []
        for g in range(groups):
            ids = sub + 8 * g
            pivot = jnp.sum(jnp.where(lane == ids, parts[g], 0.0), axis=1, keepdims=True)
            unit = jnp.where(lane < ids, parts[g], jnp.where(lane == ids, 1.0, 0.0))
            rows.append(unit * (1.0 / jnp.sqrt(pivot)))
        out.append(jnp.concatenate(rows, axis=0))
    return out


def unpack_even(got):
    two = 2 * BLK
    return got[:BLK, :BLK], got[BLK:two, BLK:], got[:BLK, BLK:], got[BLK:, :BLK], got[two:, BLK:]


def unpack_odd(got):
    two = 2 * BLK
    return got[two:, :BLK], got[BLK:two, :BLK], got[two:, BLK:], got[:BLK, :].T, got[BLK:two, BLK:].T


def whiten_kernel(total, count, damp_ref, packed_ref, out_ref):
    two = 2 * BLK
    diag = lax.broadcasted_iota(jnp.int32, (BLK, BLK), 0) == lax.broadcasted_iota(jnp.int32, (BLK, BLK), 1)
    a11, a22, a33, low, a32 = [], [], [], [], []
    for m in range(count):
        got = packed_ref[m] / total
        even = unpack_even(got)
        odd = unpack_odd(got)
        if count % 2 == 0:
            d1, d2, d3, left, corner = odd if m % 2 else even
        else:
            turn = (lax.axis_index("head") * lax.axis_size("dp") + lax.axis_index("dp")) * count + m
            d1, d2, d3, left, corner = (jnp.where(turn % 2 == 0, a, b) for a, b in zip(even, odd))
        trace = jnp.sum(jnp.where(diag, d1 + d2 + d3, 0.0), axis=(0, 1), keepdims=True)
        level = trace / HD + 1e-06
        shift = jnp.where(diag, damp_ref[m] * level, 0.0)
        a11.append(d1 + shift)
        a22.append(d2 + shift)
        a33.append(d3 + shift)
        low.append(left)
        a32.append(corner)
    each = range(count)
    w11 = inverse_factors(a11)
    l1 = [dot_t(low[m], w11[m]) for m in each]
    square = [dot_t(l1[m], l1[m]) for m in each]
    w22 = inverse_factors([a22[m] - square[m][:BLK, :BLK] for m in each])
    l32 = [dot_t(a32[m] - square[m][BLK:, :BLK], w22[m]) for m in each]
    w33 = inverse_factors([a33[m] - square[m][BLK:, BLK:] - dot_t(l32[m], l32[m]) for m in each])
    for m in each:
        below = dot(l1[m], w11[m])
        w21 = -dot(w22[m], below[:BLK])
        w32 = -dot(w33[m], dot(l32[m], w22[m]))
        w31 = -dot(w33[m], below[BLK:] + dot(l32[m], w21))
        out_ref[m, :BLK] = jnp.concatenate((w11[m], w33[m]), axis=1)
        out_ref[m, BLK:two] = jnp.concatenate((w21, w22[m]), axis=1)
        out_ref[m, two:] = jnp.concatenate((w31, w32), axis=1)


def whiten(packed, damp, total):
    count = packed.shape[0]
    return pl.pallas_call(
        functools.partial(whiten_kernel, total, count),
        in_specs=[pl.BlockSpec(memory_space=pltpu.SMEM), pl.BlockSpec(memory_space=pltpu.VMEM)],
        out_specs=pl.BlockSpec(memory_space=pltpu.VMEM),
        out_shape=jax.ShapeDtypeStruct(packed.shape, jnp.float32),
    )(damp, packed)


def remote(src, dst, send, recv, device):
    return pltpu.make_async_remote_copy(
        src_ref=src, dst_ref=dst, send_sem=send, recv_sem=recv, device_id=device, device_id_type=pl.DeviceIdType.MESH
    )


def greet(devices):
    barrier = pltpu.get_barrier_semaphore()
    for device in devices:
        pl.semaphore_signal(barrier, inc=1, device_id=device, device_id_type=pl.DeviceIdType.MESH)
    pl.semaphore_wait(barrier, len(devices))


RING = 4
HALF = BLK // 2
FAR_FIRST = (2, 1, 3, 0)
ORDERS = ((0, 1, 2), (1, 2, 0), (2, 0, 1))
AHEAD = 2
VISITS = sorted(
    ((a, b) for a in range(RING) for b in range(RING)),
    key=lambda s: ((s[0] != 2) + (s[1] != 2), (s[0] == 0) + (s[1] == 0)),
)


def place():
    head = lax.axis_index("head")
    dp = lax.axis_index("dp")
    return head // 4, head // 2 % 2 * 2 + dp // RING, dp % RING, head % 2


def neighbour(axis, step):
    spot = list(place())
    spot[axis] = (spot[axis] + step) % RING
    x, y, z, core = spot
    return {"head": (x * 2 + y // 2) * 2 + core, "dp": y % 2 * RING + z}


class Stage:
    def __init__(self, part, level, acc, far, near, sem_far, sem_near, sem_send):
        self.part, self.level, self.acc, self.far, self.near = part, level, acc, far, near
        self.sem_far, self.sem_near, self.sem_send = sem_far, sem_near, sem_send
        self.axis = ORDERS[part][level]
        self.free = ORDERS[part][level + 1 :]
        self.to = [neighbour(self.axis, 1), neighbour(self.axis, -1)]

    def pick(self, block, sub):
        spot = [sub.get(a, pl.ds(0, RING)) if a in self.free else pl.ds(0, 1) for a in range(3)]
        spot[self.axis] = pl.ds(block, 1)
        return tuple(spot)

    def rows(self, half):
        return (pl.ds(self.part * BLK + half * HALF, HALF),)

    def far_copy(self, d, sub):
        return remote(
            self.acc.at[self.pick(2, sub) + self.rows(d)],
            self.far.at[(d,) + self.pick(0, sub)],
            self.sem_send.at[0, d],
            self.sem_far.at[d],
            self.to[d],
        )

    def direct_copy(self, d, sub):
        return remote(
            self.acc.at[self.pick((1, 3)[d], sub) + self.rows(1 - d)],
            self.near.at[(d,) + self.pick(0, sub) + (pl.ds((1 - d) * HALF, HALF),)],
            self.sem_send.at[1, d],
            self.sem_near.at[d, RING],
            self.to[d],
        )

    def near_copy(self, d, sub, group):
        return remote(
            self.acc.at[self.pick((1, 3)[d], sub) + self.rows(d)],
            self.near.at[(d,) + self.pick(0, sub) + (pl.ds(d * HALF, HALF),)],
            self.sem_send.at[2, d],
            self.sem_near.at[d, group],
            self.to[d],
        )

    def groups(self):
        if not self.free:
            return [(0, {})]
        return [(g, {self.free[0]: pl.ds(g, 1)}) for g in FAR_FIRST]

    def relay(self, d, group, sub):
        mine = self.pick((1, 3)[d], sub) + self.rows(d)
        self.acc[mine] += self.far[(d,) + self.pick(0, sub)]
        self.near_copy(d, sub, group).start()

    def settle(self, group, sub):
        for d in (0, 1):
            self.near_copy(d, sub, group).wait_recv()
        mine = self.pick(0, sub)
        size = [RING if len(self.free) > 1 and a == self.free[1] else 1 for a in range(3)]
        for i in range(max(size)):
            part = list(mine)
            if len(self.free) > 1:
                part[self.free[1]] = pl.ds(i, 1)
            part = tuple(part)
            rows = (pl.ds(self.part * BLK, BLK),)
            self.acc[part + rows] += self.near[(0,) + part] + self.near[(1,) + part]

    def finish(self):
        for d in (0, 1):
            self.far_copy(d, {}).wait_send()
            self.direct_copy(d, {}).wait_send()
            self.near_copy(d, {}, 0).wait_send()


def stage_shapes(level, part):
    free = ORDERS[part][level + 1 :]
    return tuple(RING if a in free else 1 for a in range(3))


def scatter_kernel(rows_ref, weights_ref, out_ref, acc, sent, got, wide, columns, *rest):
    x, y, z, core = place()
    sem_in, sem_core = rest[-2:]
    stages = [[Stage(part, level, acc, *rest[5 * (3 * level + part) :][:5]) for part in range(3)] for level in range(3)]
    span = RING * HD
    partner = {"head": lax.axis_index("head") // 2 * 2 + 1 - core}
    count = len(VISITS)
    trips = [(0, 0)]
    for i in range(count):
        trips += [(i + 1, 0)] * (i + 1 < count) + [(i, 1)]

    def fetch(v):
        i, own = trips[v]
        to_x, to_y = (x + VISITS[i][0]) % RING, (y + VISITS[i][1]) % RING
        to_core = core if own else 1 - core
        first = ((to_x * 2 + to_y // 2) * 2 + to_core) * 8 + to_y % 2 * RING
        start = pl.multiple_of(first * HD, 2 * BLK)
        slot = v % (AHEAD + 1)
        return pltpu.make_async_copy(rows_ref.at[:, pl.ds(start, span)], columns.at[slot], sem_in.at[slot])

    for v in range(AHEAD):
        fetch(v).start()
    wide[...] = jnp.broadcast_to(weights_ref[...], wide.shape)

    def multiply(v, out):
        if v + AHEAD < len(trips):
            fetch(v + AHEAD).start()
        fetch(v).wait()

        def pair(i, carry):
            start = pl.multiple_of(i * 2 * HD, 2 * BLK)
            even = (2 * i + RING - z) % RING
            store_pair(columns[v % (AHEAD + 1), :, pl.ds(start, 2 * HD)], wide[...], out, even, (even + 1) % RING)
            return carry

        lax.fori_loop(0, RING // 2, pair, 0, unroll=True)

    def exchange(i):
        return remote(sent.at[i], got.at[i], sem_core.at[0, i], sem_core.at[1, i], partner)

    def release(i):
        a, b = VISITS[i]
        exchange(i).wait_recv()

        def add(m, carry):
            acc[a, b, m] += got[i, m]
            return carry

        lax.fori_loop(0, RING, add, 0)
        spots = ({1: pl.ds(b, 1)}, {0: pl.ds(a, 1)}, {0: pl.ds(a, 1), 1: pl.ds(b, 1)})
        for stage, at, sub in zip(stages[0], (a, b, None), spots):
            for d in (0, 1):
                if at in (2, None):
                    stage.far_copy(d, sub).start()
            for d in (0, 1):
                if at in ((1, 3)[d], None):
                    stage.direct_copy(d, sub).start()

    for v, (i, own) in enumerate(trips):
        if own:
            multiply(v, acc.at[VISITS[i]])
            if i:
                release(i - 1)
        else:
            multiply(v, sent.at[i])
            if v == 0:
                greet([partner] + [to for stage in stages[0] for to in stage.to])
            exchange(i).start()
    release(count - 1)
    for level in range(3):
        now = stages[level]
        for stage in now:
            for d in (0, 1):
                stage.far_copy(d, {}).wait_recv()
                for group, sub in stage.groups():
                    stage.relay(d, group, sub)
        for stage in now:
            for d in (0, 1):
                stage.direct_copy(d, {}).wait_recv()
        for n in range(len(now[0].groups())):
            for part in range(3):
                group, sub = now[part].groups()[n]
                now[part].settle(group, sub)
                if level < 2:
                    later = stages[level + 1][part]
                    if group == 2:
                        later.far_copy(0, {}).start()
                        later.far_copy(1, {}).start()
                    elif group:
                        later.direct_copy(group // 2, {}).start()
    out_ref[0] = acc[0, 0, 0]
    for i in range(count):
        exchange(i).wait_send()
    for level in stages:
        for stage in level:
            stage.finish()


def gram_sums(projected, weights):
    tokens, width = projected.shape
    rows, lanes = HD, 2 * BLK
    f32 = jnp.float32
    rings = []
    for level in range(3):
        for part in range(3):
            shape = stage_shapes(level, part)
            rings += [
                pltpu.VMEM((2,) + shape + (HALF, lanes), f32),
                pltpu.VMEM((2,) + shape + (BLK, lanes), f32),
                pltpu.SemaphoreType.DMA((2,)),
                pltpu.SemaphoreType.DMA((2, RING + 1)),
                pltpu.SemaphoreType.DMA((3, 2)),
            ]
    return pl.pallas_call(
        scatter_kernel,
        in_specs=[pl.BlockSpec(memory_space=pl.ANY), pl.BlockSpec(memory_space=pltpu.VMEM)],
        out_specs=pl.BlockSpec(memory_space=pltpu.VMEM),
        out_shape=jax.ShapeDtypeStruct((1, rows, lanes), f32),
        scratch_shapes=[
            pltpu.VMEM((RING, RING, RING, rows, lanes), f32),
            pltpu.VMEM((len(VISITS), RING, rows, lanes), f32),
            pltpu.VMEM((len(VISITS), RING, rows, lanes), f32),
            pltpu.VMEM((tokens, 2 * HD), projected.dtype),
            pltpu.VMEM((AHEAD + 1, tokens, RING * HD), projected.dtype),
            *rings,
            pltpu.SemaphoreType.DMA((AHEAD + 1,)),
            pltpu.SemaphoreType.DMA((2, len(VISITS))),
        ],
        compiler_params=pltpu.CompilerParams(collective_id=0, has_side_effects=True, vmem_limit_bytes=60 << 20),
    )(projected, weights)


def gather_kernel(n_dp, share, packed_ref, out_ref, got, sems):
    dp = lax.axis_index("dp")
    peers = [lax.rem(dp + o, n_dp) for o in range(1, n_dp)]
    greet([{"dp": peer} for peer in peers])
    flight = []
    for o, peer in enumerate(peers):
        copy = remote(packed_ref, got.at[o], sems.at[0, o], sems.at[1, o], {"dp": peer})
        copy.start()
        flight.append(copy)
    two = 2 * BLK

    def unpack(source, base):
        def one(m, carry):
            top = source[m, :BLK]
            out_ref[base + m, :BLK, :two] = jnp.where(lax.broadcasted_iota(jnp.int32, (BLK, two), 1) < BLK, top, 0.0)
            out_ref[base + m, BLK:, :two] = source[m, BLK:]
            out_ref[base + m, :two, two:] = jnp.zeros((two, BLK), jnp.float32)
            out_ref[base + m, two:, two:] = top[:, BLK:]
            return carry

        lax.fori_loop(0, share, one, 0)

    unpack(packed_ref, dp * share)
    for o in range(n_dp - 1):
        flight[o].wait()
        unpack(got.at[o], lax.rem(dp + n_dp - 1 - o, n_dp) * share)


def gather(packed, n_dp):
    share, rows, lanes = packed.shape
    return pl.pallas_call(
        functools.partial(gather_kernel, n_dp, share),
        in_specs=[pl.BlockSpec(memory_space=pltpu.VMEM)],
        out_specs=pl.BlockSpec(memory_space=pltpu.VMEM),
        out_shape=jax.ShapeDtypeStruct((n_dp * share, HD, HD), jnp.float32),
        scratch_shapes=[
            pltpu.VMEM((n_dp - 1, share, rows, lanes), jnp.float32),
            pltpu.SemaphoreType.DMA((2, n_dp - 1)),
        ],
        compiler_params=pltpu.CompilerParams(collective_id=1, has_side_effects=True),
    )(packed)


def on_device(projected, weight_exp, damp_exp):
    n_head = lax.axis_size("head")
    n_dp = lax.axis_size("dp")
    mats = projected.shape[1] // HD
    share = mats // (n_head * n_dp)
    total = projected.shape[0] * n_head * n_dp
    weights = jnp.exp2(weight_exp.astype(jnp.float32)).astype(jnp.bfloat16)
    owned = gram_sums(projected, weights[:, None])
    first = (lax.axis_index("head") * n_dp + lax.axis_index("dp")) * share
    damp = jnp.exp2(-lax.dynamic_slice_in_dim(damp_exp, first, share, 0).astype(jnp.float32))
    factors = whiten(owned, damp, float(total))
    return gather(factors, n_dp)


def solution(mesh):
    return jax.shard_map(
        on_device,
        mesh=mesh,
        in_specs=(P(("dp", "head"), None), P(("dp", "head")), P()),
        out_specs=P("head", None, None),
        check_vma=False,
    )
```

```python
import functools

import jax
import jax.numpy as jnp
from jax import lax
from jax.experimental import pallas as pl
from jax.experimental.pallas import tpu as pltpu
from jax.sharding import PartitionSpec as P

HD = 192
BLK = HD // 3
HIGH = lax.Precision.HIGHEST


def store_pair(rows, wide, out, at, after):
    weighted = rows * wide
    contract = (((0,), (0,)), ((), ()))
    width = 4 * BLK
    first = lax.dot_general(rows[:, :width], weighted[:, :width], contract, preferred_element_type=jnp.float32)
    second = lax.dot_general(rows[:, -width:], weighted[:, -width:], contract, preferred_element_type=jnp.float32)
    two = 2 * BLK
    lanes = lax.broadcasted_iota(jnp.int32, (BLK, two), 1)
    corner = pltpu.roll(first[two : two + BLK, two:], BLK, 1)
    out[at, :BLK, :] = jnp.where(lanes < BLK, first[:BLK, :two], corner)
    out[at, BLK:, :] = first[BLK:HD, :two]
    out[after, :two, :] = second[BLK : BLK + two, two:]
    corner = pltpu.roll(second[BLK:two, :two], BLK, 1)
    out[after, two:, :] = jnp.where(lanes < BLK, corner, second[HD:, two:])


def dot(a, b):
    return lax.dot_general(a, b, (((1,), (0,)), ((), ())), precision=HIGH, preferred_element_type=jnp.float32)


def dot_t(a, b):
    return lax.dot_general(a, b, (((1,), (1,)), ((), ())), precision=HIGH, preferred_element_type=jnp.float32)


PANEL = 8


def inverse_factor(block):
    lane = lax.broadcasted_iota(jnp.int32, (PANEL, BLK), 1)
    sub = lax.broadcasted_iota(jnp.int32, (PANEL, BLK), 0)
    groups = BLK // PANEL
    each = range(PANEL)
    parts = [block[PANEL * g : PANEL * g + PANEL] for g in range(groups)]
    whole = (PANEL, BLK)
    for p in range(groups):
        first = PANEL * p
        columns = {g: [jnp.broadcast_to(parts[g][:, first + j : first + j + 1], whole) for j in each] for g in range(p, groups)}
        low = [[jnp.broadcast_to(columns[p][j][i : i + 1], whole) for j in range(i + 1)] for i in each]
        inside = (lane >= first) & (lane < first + PANEL)
        rows = []
        for i in each:
            own = jnp.where(inside, jnp.where(lane == first + i, 1.0, 0.0), jnp.broadcast_to(parts[p][i : i + 1], whole))
            rows.append(own)
        scale = []
        for k in each:
            inverse = 1.0 / low[k][k]
            scale.append(inverse)
            raw = {i: low[i][k] for i in range(k, PANEL)}
            for i in range(k + 1, PANEL):
                ratio = raw[i] * inverse
                for j in range(k + 1, i + 1):
                    low[i][j] = low[i][j] - ratio * raw[j]
                rows[i] = rows[i] - ratio * rows[k]
                low[i][k] = ratio
        done = jnp.zeros(whole, jnp.float32)
        for i in each:
            done = jnp.where((sub == i) & (lane <= first + i), rows[i] * lax.rsqrt(low[i][i]), done)
        if p + 1 < groups:
            solved = [None] * PANEL
            for k in reversed(each):
                value = rows[k] * scale[k]
                for i in range(k + 1, PANEL):
                    value = value - low[i][k] * solved[i]
                solved[k] = value
            for g in range(p + 1, groups):
                terms = [columns[g][j] * solved[j] for j in each]
                while len(terms) > 1:
                    terms = [a + b for a, b in zip(terms[::2], terms[1::2])]
                parts[g] = jnp.where(inside, 0.0, parts[g]) - terms[0]
        parts[p] = done
    return jnp.concatenate(parts, axis=0)


def inverse_factors(blocks):
    return [inverse_factor(block) for block in blocks]


def unpack_even(got):
    two = 2 * BLK
    return got[:BLK, :BLK], got[BLK:two, BLK:], got[:BLK, BLK:], got[BLK:, :BLK], got[two:, BLK:]


def unpack_odd(got):
    two = 2 * BLK
    return got[two:, :BLK], got[BLK:two, :BLK], got[two:, BLK:], got[:BLK, :].T, got[BLK:two, BLK:].T


def whiten_kernel(total, count, damp_ref, packed_ref, out_ref):
    two = 2 * BLK
    diag = lax.broadcasted_iota(jnp.int32, (BLK, BLK), 0) == lax.broadcasted_iota(jnp.int32, (BLK, BLK), 1)
    a11, a22, a33, low, a32 = [], [], [], [], []
    for m in range(count):
        got = packed_ref[m] / total
        even = unpack_even(got)
        odd = unpack_odd(got)
        if count % 2 == 0:
            d1, d2, d3, left, corner = odd if m % 2 else even
        else:
            turn = (lax.axis_index("head") * lax.axis_size("dp") + lax.axis_index("dp")) * count + m
            d1, d2, d3, left, corner = (jnp.where(turn % 2 == 0, a, b) for a, b in zip(even, odd))
        trace = jnp.sum(jnp.where(diag, d1 + d2 + d3, 0.0), axis=(0, 1), keepdims=True)
        level = trace / HD + 1e-06
        shift = jnp.where(diag, damp_ref[m] * level, 0.0)
        a11.append(d1 + shift)
        a22.append(d2 + shift)
        a33.append(d3 + shift)
        low.append(left)
        a32.append(corner)
    each = range(count)
    w11 = inverse_factors(a11)
    l1 = [dot_t(low[m], w11[m]) for m in each]
    square = [dot_t(l1[m], l1[m]) for m in each]
    w22 = inverse_factors([a22[m] - square[m][:BLK, :BLK] for m in each])
    l32 = [dot_t(a32[m] - square[m][BLK:, :BLK], w22[m]) for m in each]
    w33 = inverse_factors([a33[m] - square[m][BLK:, BLK:] - dot_t(l32[m], l32[m]) for m in each])
    for m in each:
        below = dot(l1[m], w11[m])
        w21 = -dot(w22[m], below[:BLK])
        w32 = -dot(w33[m], dot(l32[m], w22[m]))
        w31 = -dot(w33[m], below[BLK:] + dot(l32[m], w21))
        out_ref[m, :BLK] = jnp.concatenate((w11[m], w33[m]), axis=1)
        out_ref[m, BLK:two] = jnp.concatenate((w21, w22[m]), axis=1)
        out_ref[m, two:] = jnp.concatenate((w31, w32), axis=1)


def whiten(packed, damp, total):
    count = packed.shape[0]
    return pl.pallas_call(
        functools.partial(whiten_kernel, total, count),
        in_specs=[pl.BlockSpec(memory_space=pltpu.SMEM), pl.BlockSpec(memory_space=pltpu.VMEM)],
        out_specs=pl.BlockSpec(memory_space=pltpu.VMEM),
        out_shape=jax.ShapeDtypeStruct(packed.shape, jnp.float32),
    )(damp, packed)


def remote(src, dst, send, recv, device):
    return pltpu.make_async_remote_copy(
        src_ref=src, dst_ref=dst, send_sem=send, recv_sem=recv, device_id=device, device_id_type=pl.DeviceIdType.MESH
    )


def greet(devices):
    barrier = pltpu.get_barrier_semaphore()
    for device in devices:
        pl.semaphore_signal(barrier, inc=1, device_id=device, device_id_type=pl.DeviceIdType.MESH)
    pl.semaphore_wait(barrier, len(devices))


RING = 4
HALF = BLK // 2
FAR_FIRST = (2, 1, 3, 0)
ORDERS = ((0, 1, 2), (1, 2, 0), (2, 0, 1))
AHEAD = 6
LAG = 4
VISITS = ((2, 2), (2, 1), (1, 2), (2, 3), (3, 2), (2, 0), (0, 2), (1, 1), (1, 3), (3, 1), (3, 3), (1, 0), (3, 0), (0, 1), (0, 3), (0, 0))


def place():
    head = lax.axis_index("head")
    dp = lax.axis_index("dp")
    return head // 4, head // 2 % 2 * 2 + dp // RING, dp % RING, head % 2


def neighbour(axis, step):
    spot = list(place())
    spot[axis] = (spot[axis] + step) % RING
    x, y, z, core = spot
    return {"head": (x * 2 + y // 2) * 2 + core, "dp": y % 2 * RING + z}


def slots_of(level, part):
    return RING ** (1 + (part == 2)) if level == 0 else RING


class Stage:
    def __init__(self, part, level, acc, far, near, sem_far, sem_near, sem_send):
        self.part, self.level, self.acc, self.far, self.near = part, level, acc, far, near
        self.sem_far, self.sem_near, self.sem_send = sem_far, sem_near, sem_send
        self.axis = ORDERS[part][level]
        self.free = ORDERS[part][level + 1 :]
        self.to = [neighbour(self.axis, 1), neighbour(self.axis, -1)]
        self.slots = slots_of(level, part)

    def pick(self, block, sub):
        spot = [sub.get(a, pl.ds(0, RING)) if a in self.free else pl.ds(0, 1) for a in range(3)]
        spot[self.axis] = pl.ds(block, 1)
        return tuple(spot)

    def rows(self, half):
        return (pl.ds(self.part * BLK + half * HALF, HALF),)

    def far_copy(self, d, sub, slot=0):
        return remote(
            self.acc.at[self.pick(2, sub) + self.rows(d)],
            self.far.at[(d,) + self.pick(0, sub)],
            self.sem_send.at[0, d],
            self.sem_far.at[d, slot],
            self.to[d],
        )

    def direct_copy(self, d, sub):
        return remote(
            self.acc.at[self.pick((1, 3)[d], sub) + self.rows(1 - d)],
            self.near.at[(d,) + self.pick(0, sub) + (pl.ds((1 - d) * HALF, HALF),)],
            self.sem_send.at[1, d],
            self.sem_near.at[d, self.slots],
            self.to[d],
        )

    def near_copy(self, d, sub, group):
        return remote(
            self.acc.at[self.pick((1, 3)[d], sub) + self.rows(d)],
            self.near.at[(d,) + self.pick(0, sub) + (pl.ds(d * HALF, HALF),)],
            self.sem_send.at[2, d],
            self.sem_near.at[d, group],
            self.to[d],
        )

    def groups(self):
        if not self.free:
            return [(0, {})]
        return [(g, {self.free[0]: pl.ds(g, 1)}) for g in FAR_FIRST]

    def relay(self, d, sub):
        mine = self.pick((1, 3)[d], sub) + self.rows(d)
        self.acc[mine] += self.far[(d,) + self.pick(0, sub)]

    def settle(self, sub):
        mine = self.pick(0, sub)
        size = [RING if len(self.free) > 1 and a == self.free[1] else 1 for a in range(3)]
        for i in range(max(size)):
            part = list(mine)
            if len(self.free) > 1:
                part[self.free[1]] = pl.ds(i, 1)
            part = tuple(part)
            rows = (pl.ds(self.part * BLK, BLK),)
            self.acc[part + rows] += self.near[(0,) + part] + self.near[(1,) + part]

    def finish(self):
        for d in (0, 1):
            self.far_copy(d, {}).wait_send()
            self.direct_copy(d, {}).wait_send()
            self.near_copy(d, {}, 0).wait_send()


def stage_shapes(level, part):
    free = ORDERS[part][level + 1 :]
    return tuple(RING if a in free else 1 for a in range(3))


def scatter_kernel(rows_ref, weights_ref, out_ref, acc, sent, got, mine, wide, columns, *rest):
    x, y, z, core = place()
    sem_in, sem_core = rest[-2:]
    stages = [[Stage(part, level, acc, *rest[5 * (3 * level + part) :][:5]) for part in range(3)] for level in range(3)]
    span = RING * HD
    partner = {"head": lax.axis_index("head") // 2 * 2 + 1 - core}
    count = len(VISITS)
    index = {spot: i for i, spot in enumerate(VISITS)}
    trips = [(0, 0)]
    for i in range(count):
        trips += [(i + 1, 0)] * (i + 1 < count) + [(i, 1)]
    turn = {trip: v for v, trip in enumerate(trips)}

    def fetch(v):
        i, own = trips[v]
        to_x, to_y = (x + VISITS[i][0]) % RING, (y + VISITS[i][1]) % RING
        to_core = core if own else 1 - core
        first = ((to_x * 2 + to_y // 2) * 2 + to_core) * 8 + to_y % 2 * RING
        start = pl.multiple_of(first * HD, 2 * BLK)
        slot = v % AHEAD
        return pltpu.make_async_copy(rows_ref.at[:, pl.ds(start, span)], columns.at[slot], sem_in.at[slot])

    for v in range(AHEAD):
        fetch(v).start()
    wide[...] = jnp.broadcast_to(weights_ref[...], wide.shape)

    def multiply(v, out):
        for i in range(RING // 2):
            even = (2 * i + RING - z) % RING
            store_pair(columns[v % AHEAD, :, 2 * i * HD : 2 * (i + 1) * HD], wide[...], out, even, (even + 1) % RING)

    def exchange(i):
        return remote(sent.at[i], got.at[i], sem_core.at[0, i], sem_core.at[1, i], partner)

    def spots(i):
        a, b = VISITS[i]
        return ((a, {1: pl.ds(b, 1)}, b), (b, {0: pl.ds(a, 1)}, a), (None, {0: pl.ds(a, 1), 1: pl.ds(b, 1)}, RING * a + b))

    relays = {}
    for i in range(count):
        for part, (at, sub, slot) in enumerate(spots(i)):
            for d in (0, 1):
                if at in ((1, 3)[d], None):
                    source = VISITS[i] if at is None else tuple(2 if n == part else VISITS[i][n] for n in range(2))
                    when = max(i + 2, index[source] + LAG)
                    relays.setdefault(when, []).append((stages[0][part], d, sub, slot))

    for r in range(-1, max(relays) + 1):
        now = [turn[trip] for trip in ((r + 1, 0), (r, 1)) if trip in turn]
        for v in now:
            fetch(v).wait()
        if 1 <= r <= count:
            exchange(r - 1).wait_recv()
        moved = relays.get(r, [])
        for stage, d, sub, slot in moved:
            stage.far_copy(d, sub, slot).wait_recv()
        for v in now:
            i, own = trips[v]
            multiply(v, mine.at[i % 2] if own else sent.at[i])
        if 1 <= r <= count:
            a, b = VISITS[r - 1]
            acc[a, b] = mine[(r - 1) % 2] + got[r - 1]
        for stage, d, sub, slot in moved:
            stage.relay(d, sub)
        if r == -1:
            greet([partner] + [to for stage in stages[0] for to in stage.to])
        if r + 1 < count:
            exchange(r + 1).start()
        for v in now:
            if v + AHEAD < len(trips):
                fetch(v + AHEAD).start()
        if 1 <= r <= count:
            for stage, (at, sub, slot) in zip(stages[0], spots(r - 1)):
                for d in (0, 1):
                    if at in (2, None):
                        stage.far_copy(d, sub, slot).start()
        for stage, d, sub, slot in moved:
            stage.near_copy(d, sub, slot).start()
        if 1 <= r <= count:
            for stage, (at, sub, slot) in zip(stages[0], spots(r - 1)):
                for d in (0, 1):
                    if at in ((1, 3)[d], None):
                        stage.direct_copy(d, sub).start()

    for level in range(3):
        now = stages[level]
        if level:
            for stage in now:
                for d in (0, 1):
                    stage.far_copy(d, {}).wait_recv()
                    for group, sub in stage.groups():
                        stage.relay(d, sub)
                        stage.near_copy(d, sub, group).start()
        for stage in now:
            for d in (0, 1):
                stage.direct_copy(d, {}).wait_recv()
        for n in range(len(now[0].groups())):
            for part in range(3):
                group, sub = now[part].groups()[n]
                if level or part == 0:
                    arrivals = [(sub, group)]
                elif part == 1:
                    arrivals = [({0: pl.ds(a, 1)}, a) for a in range(RING) if n == 0]
                else:
                    arrivals = [({0: pl.ds(group, 1), 1: pl.ds(b, 1)}, RING * group + b) for b in range(RING)]
                for at, slot in arrivals:
                    for d in (0, 1):
                        now[part].near_copy(d, at, slot).wait_recv()
                now[part].settle(sub)
                if level < 2:
                    later = stages[level + 1][part]
                    if group == 2:
                        later.far_copy(0, {}).start()
                        later.far_copy(1, {}).start()
                    elif group:
                        later.direct_copy(group // 2, {}).start()
    out_ref[0] = acc[0, 0, 0]
    for i in range(count):
        exchange(i).wait_send()
    for level in stages:
        for stage in level:
            stage.finish()


def gram_sums(projected, weights):
    tokens, width = projected.shape
    rows, lanes = HD, 2 * BLK
    f32 = jnp.float32
    rings = []
    for level in range(3):
        for part in range(3):
            shape = stage_shapes(level, part)
            rings += [
                pltpu.VMEM((2,) + shape + (HALF, lanes), f32),
                pltpu.VMEM((2,) + shape + (BLK, lanes), f32),
                pltpu.SemaphoreType.DMA((2, slots_of(level, part))),
                pltpu.SemaphoreType.DMA((2, slots_of(level, part) + 1)),
                pltpu.SemaphoreType.DMA((3, 2)),
            ]
    return pl.pallas_call(
        scatter_kernel,
        in_specs=[pl.BlockSpec(memory_space=pl.ANY), pl.BlockSpec(memory_space=pltpu.VMEM)],
        out_specs=pl.BlockSpec(memory_space=pltpu.VMEM),
        out_shape=jax.ShapeDtypeStruct((1, rows, lanes), f32),
        scratch_shapes=[
            pltpu.VMEM((RING, RING, RING, rows, lanes), f32),
            pltpu.VMEM((len(VISITS), RING, rows, lanes), f32),
            pltpu.VMEM((len(VISITS), RING, rows, lanes), f32),
            pltpu.VMEM((2, RING, rows, lanes), f32),
            pltpu.VMEM((tokens, 2 * HD), projected.dtype),
            pltpu.VMEM((AHEAD, tokens, RING * HD), projected.dtype),
            *rings,
            pltpu.SemaphoreType.DMA((AHEAD,)),
            pltpu.SemaphoreType.DMA((2, len(VISITS))),
        ],
        compiler_params=pltpu.CompilerParams(collective_id=0, has_side_effects=True, vmem_limit_bytes=60 << 20),
    )(projected, weights)


def gather_kernel(n_dp, share, packed_ref, out_ref, got, sems):
    dp = lax.axis_index("dp")
    peers = [lax.rem(dp + o, n_dp) for o in range(1, n_dp)]
    greet([{"dp": peer} for peer in peers])
    flight = []
    for o, peer in enumerate(peers):
        copy = remote(packed_ref, got.at[o], sems.at[0, o], sems.at[1, o], {"dp": peer})
        copy.start()
        flight.append(copy)
    two = 2 * BLK

    def unpack(source, base):
        def one(m, carry):
            top = source[m, :BLK]
            out_ref[base + m, :BLK, :two] = jnp.where(lax.broadcasted_iota(jnp.int32, (BLK, two), 1) < BLK, top, 0.0)
            out_ref[base + m, BLK:, :two] = source[m, BLK:]
            out_ref[base + m, :two, two:] = jnp.zeros((two, BLK), jnp.float32)
            out_ref[base + m, two:, two:] = top[:, BLK:]
            return carry

        lax.fori_loop(0, share, one, 0)

    unpack(packed_ref, dp * share)
    for o in range(n_dp - 1):
        flight[o].wait()
        unpack(got.at[o], lax.rem(dp + n_dp - 1 - o, n_dp) * share)


def gather(packed, n_dp):
    share, rows, lanes = packed.shape
    return pl.pallas_call(
        functools.partial(gather_kernel, n_dp, share),
        in_specs=[pl.BlockSpec(memory_space=pltpu.VMEM)],
        out_specs=pl.BlockSpec(memory_space=pltpu.VMEM),
        out_shape=jax.ShapeDtypeStruct((n_dp * share, HD, HD), jnp.float32),
        scratch_shapes=[
            pltpu.VMEM((n_dp - 1, share, rows, lanes), jnp.float32),
            pltpu.SemaphoreType.DMA((2, n_dp - 1)),
        ],
        compiler_params=pltpu.CompilerParams(collective_id=1, has_side_effects=True),
    )(packed)


def on_device(projected, weight_exp, damp_exp):
    n_head = lax.axis_size("head")
    n_dp = lax.axis_size("dp")
    mats = projected.shape[1] // HD
    share = mats // (n_head * n_dp)
    total = projected.shape[0] * n_head * n_dp
    weights = jnp.exp2(weight_exp.astype(jnp.float32)).astype(jnp.bfloat16)
    owned = gram_sums(projected, weights[:, None])
    first = (lax.axis_index("head") * n_dp + lax.axis_index("dp")) * share
    damp = jnp.exp2(-lax.dynamic_slice_in_dim(damp_exp, first, share, 0).astype(jnp.float32))
    factors = whiten(owned, damp, float(total))
    return gather(factors, n_dp)


def solution(mesh):
    return jax.shard_map(
        on_device,
        mesh=mesh,
        in_specs=(P(("dp", "head"), None), P(("dp", "head")), P()),
        out_specs=P("head", None, None),
        check_vma=False,
    )
```

```python
import functools

import jax
import jax.numpy as jnp
from jax import lax
from jax.experimental import pallas as pl
from jax.experimental.pallas import tpu as pltpu
from jax.sharding import PartitionSpec as P

HD = 192
BLK = HD // 3
HIGH = lax.Precision.HIGHEST


def store_pair(rows, wide, out, at, after):
    weighted = rows * wide
    contract = (((0,), (0,)), ((), ()))
    width = 4 * BLK
    first = lax.dot_general(rows[:, :width], weighted[:, :width], contract, preferred_element_type=jnp.float32)
    second = lax.dot_general(rows[:, -width:], weighted[:, -width:], contract, preferred_element_type=jnp.float32)
    two = 2 * BLK
    lanes = lax.broadcasted_iota(jnp.int32, (BLK, two), 1)
    corner = pltpu.roll(first[two : two + BLK, two:], BLK, 1)
    out[at, :BLK, :] = jnp.where(lanes < BLK, first[:BLK, :two], corner)
    out[at, BLK:, :] = first[BLK:HD, :two]
    out[after, :two, :] = second[BLK : BLK + two, two:]
    corner = pltpu.roll(second[BLK:two, :two], BLK, 1)
    out[after, two:, :] = jnp.where(lanes < BLK, corner, second[HD:, two:])


def dot(a, b):
    return lax.dot_general(a, b, (((1,), (0,)), ((), ())), precision=HIGH, preferred_element_type=jnp.float32)


def dot_t(a, b):
    return lax.dot_general(a, b, (((1,), (1,)), ((), ())), precision=HIGH, preferred_element_type=jnp.float32)


PANEL = 8


def inverse_factor(block):
    lane = lax.broadcasted_iota(jnp.int32, (PANEL, BLK), 1)
    sub = lax.broadcasted_iota(jnp.int32, (PANEL, BLK), 0)
    groups = BLK // PANEL
    each = range(PANEL)
    whole = (PANEL, BLK)
    parts = [block[PANEL * g : PANEL * g + PANEL] for g in range(groups)]

    def spread(part, at):
        return [jnp.broadcast_to(part[:, at + j : at + j + 1], whole) for j in each]

    def total(terms):
        while len(terms) > 1:
            terms = [a + b for a, b in zip(terms[::2], terms[1::2])]
        return terms[0]

    own = spread(parts[0], 0)
    for p in range(groups):
        first = PANEL * p
        columns = {g: spread(parts[g], first) for g in range(p + 1, groups)}
        ahead = spread(parts[p + 1], first + PANEL) if p + 1 < groups else None
        low = [[jnp.broadcast_to(own[j][i : i + 1], whole) for j in range(i + 1)] for i in each]
        inside = (lane >= first) & (lane < first + PANEL)
        rows = [
            jnp.where(inside, jnp.where(lane == first + i, 1.0, 0.0), jnp.broadcast_to(parts[p][i : i + 1], whole)) for i in each
        ]
        scale = []
        for k in each:
            inverse = 1.0 / low[k][k]
            scale.append(inverse)
            raw = {i: low[i][k] for i in range(k, PANEL)}
            for i in range(k + 1, PANEL):
                ratio = raw[i] * inverse
                for j in range(k + 1, i + 1):
                    low[i][j] = low[i][j] - ratio * raw[j]
                rows[i] = rows[i] - ratio * rows[k]
                low[i][k] = ratio
        done = jnp.zeros(whole, jnp.float32)
        for i in each:
            done = jnp.where((sub == i) & (lane <= first + i), rows[i] * lax.rsqrt(low[i][i]), done)
        if p + 1 < groups:
            cross = columns[p + 1]
            lifted = []
            for k in each:
                value = cross[k]
                for j in range(k):
                    value = value - low[k][j] * lifted[j]
                lifted.append(value)
            scaled = [lifted[k] * scale[k] for k in each]
            own = [
                ahead[j] - total([scaled[k] * jnp.broadcast_to(lifted[k][j : j + 1], whole) for k in each]) for j in each
            ]
            solved = [None] * PANEL
            for k in reversed(each):
                value = rows[k] * scale[k]
                for i in range(k + 1, PANEL):
                    value = value - low[i][k] * solved[i]
                solved[k] = value
            for g in range(p + 1, groups):
                parts[g] = jnp.where(inside, 0.0, parts[g]) - total([columns[g][j] * solved[j] for j in each])
        parts[p] = done
    return jnp.concatenate(parts, axis=0)


def unpack_even(got):
    two = 2 * BLK
    return got[:BLK, :BLK], got[BLK:two, BLK:], got[:BLK, BLK:], got[BLK:, :BLK], got[two:, BLK:]


def unpack_odd(got):
    two = 2 * BLK
    return got[two:, :BLK], got[BLK:two, :BLK], got[two:, BLK:], got[:BLK, :].T, got[BLK:two, BLK:].T


def remote(src, dst, send, recv, device):
    return pltpu.make_async_remote_copy(
        src_ref=src, dst_ref=dst, send_sem=send, recv_sem=recv, device_id=device, device_id_type=pl.DeviceIdType.MESH
    )


def greet(devices):
    barrier = pltpu.get_barrier_semaphore()
    for device in devices:
        pl.semaphore_signal(barrier, inc=1, device_id=device, device_id_type=pl.DeviceIdType.MESH)
    pl.semaphore_wait(barrier, len(devices))


RING = 4
HALF = BLK // 2
FAR_FIRST = (2, 1, 3, 0)
ORDERS = ((0, 1, 2), (1, 2, 0), (2, 0, 1))
AHEAD = 6
VISIT_US = 1.0
TAIL_US = 0.2
HOP_US = 2.5
LINK_RATE = 46.6e3
VISITS = ((2, 2), (2, 1), (1, 2), (2, 3), (3, 2), (2, 0), (0, 2), (1, 0), (3, 0), (0, 0), (1, 1), (3, 3), (1, 3), (3, 1), (0, 1), (0, 3))


def place():
    head = lax.axis_index("head")
    dp = lax.axis_index("dp")
    return head // 4, head // 2 % 2 * 2 + dp // RING, dp % RING, head % 2


def neighbour(axis, step):
    spot = list(place())
    spot[axis] = (spot[axis] + step) % RING
    x, y, z, core = spot
    return {"head": (x * 2 + y // 2) * 2 + core, "dp": y % 2 * RING + z}


class First:
    def __init__(self, part, acc, far, near, sem_far, sem_near, sem_send):
        self.part, self.level, self.acc, self.far, self.near = part, 0, acc, far, near
        self.size = far.shape[1] * BLK * 2 * BLK * 4
        self.sem_far, self.sem_near, self.sem_send = sem_far, sem_near, sem_send
        self.to = [neighbour(part, 1), neighbour(part, -1)]
        self.rows = pl.ds(part * BLK, BLK)

    def parity(self, slot):
        return (slot + slot // RING) % 2

    def visit(self, block, slot):
        return ((block, slot), (slot, block), (slot // RING, slot % RING))[self.part]

    def slot(self, visit):
        a, b = visit
        return (b, a, RING * a + b)[self.part]

    def block(self, visit):
        return (visit[0], visit[1], None)[self.part]

    def at(self, block, slot):
        return self.visit(block, slot) + (pl.ds(block, 1) if self.part == 2 else pl.ds(0, RING), self.rows)

    def whole(self, block):
        spot = [pl.ds(0, RING)] * 3
        spot[self.part] = pl.ds(block, 1)
        return self.acc.at[tuple(spot) + (self.rows,)]

    def far_copy(self, slot):
        return remote(
            self.acc.at[self.at(2, slot)], self.far.at[slot], self.sem_send.at[0], self.sem_far.at[slot], self.to[self.parity(slot)]
        )

    def near_copy(self, d, slot):
        return remote(
            self.acc.at[self.at((1, 3)[d], slot)], self.near.at[d, slot], self.sem_send.at[1 + d], self.sem_near.at[d, slot], self.to[d]
        )

    def relay(self, slot):
        self.acc[self.at((1, 3)[self.parity(slot)], slot)] += self.far[slot]

    def members(self, group):
        return ([group], list(range(RING)), [RING * group + b for b in range(RING)])[self.part]

    def settle(self, group):
        for slot in self.members(group):
            if self.part == 1:
                self.acc[slot, 0, group, self.rows] += self.near[0, slot, group] + self.near[1, slot, group]
            else:
                self.acc[self.at(0, slot)] += self.near[0, slot] + self.near[1, slot]

    def finish(self):
        for sem, block in enumerate((2, 1, 3)):
            whole = self.whole(block)
            remote(whole, whole, self.sem_send.at[sem], self.sem_far.at[0], self.to[0]).wait_send()


class Later:
    def __init__(self, part, level, acc, far, near, sem_far, sem_near, sem_send):
        self.part, self.level, self.acc, self.far, self.near = part, level, acc, far, near
        self.size = (1 if level == 2 else RING) * HALF * 2 * BLK * 4
        self.sem_far, self.sem_near, self.sem_send = sem_far, sem_near, sem_send
        self.axis = ORDERS[part][level]
        self.free = ORDERS[part][level + 1 :]
        self.to = [neighbour(self.axis, 1), neighbour(self.axis, -1)]

    def pick(self, block, group):
        spot = [pl.ds(0, 1)] * 3
        for axis in self.free:
            spot[axis] = pl.ds(0, RING) if group is None else pl.ds(group, 1)
        spot[self.axis] = pl.ds(block, 1)
        return tuple(spot)

    def rows(self, half):
        return (pl.ds(self.part * BLK + half * HALF, HALF),)

    def copy(self, src, dst, send, recv, d):
        return remote(self.acc.at[src], dst, self.sem_send.at[send, d], recv, self.to[d])

    def far_copy(self, d):
        return self.copy(self.pick(2, None) + self.rows(d), self.far.at[(d,) + self.pick(0, None)], 0, self.sem_far.at[d], d)

    def direct_copy(self, d):
        half = self.near.at[(d,) + self.pick(0, None) + (pl.ds((1 - d) * HALF, HALF),)]
        return self.copy(self.pick((1, 3)[d], None) + self.rows(1 - d), half, 1, self.sem_near.at[d, RING], d)

    def near_copy(self, d, group):
        half = self.near.at[(d,) + self.pick(0, group) + (pl.ds(d * HALF, HALF),)]
        return self.copy(self.pick((1, 3)[d], group) + self.rows(d), half, 2, self.sem_near.at[d, group or 0], d)

    def groups(self):
        return FAR_FIRST if self.free else (0,)

    def relay(self, d):
        self.acc[self.pick((1, 3)[d], None) + self.rows(d)] += self.far[(d,) + self.pick(0, None)]

    def settle(self, group):
        spot = self.pick(0, group)
        self.acc[spot + (pl.ds(self.part * BLK, BLK),)] += self.near[(0,) + spot] + self.near[(1,) + spot]

    def finish(self):
        for d in (0, 1):
            for copy in (self.far_copy(d), self.direct_copy(d), self.near_copy(d, None)):
                copy.wait_send()


def scatter_kernel(rows_ref, weights_ref, out_ref, acc, sent, got, mine, wide, columns, *rest):
    x, y, z, core = place()
    sem_in, sem_core = rest[-2:]
    stages = [[(First(part, acc, *refs) if level == 0 else Later(part, level, acc, *refs)) for part in range(3) for refs in [rest[5 * (3 * level + part) :][:5]]] for level in range(3)]
    span = RING * HD
    partner = {"head": lax.axis_index("head") // 2 * 2 + 1 - core}
    count = len(VISITS)
    trips = [(0, 0)]
    for i in range(count):
        trips += [(i + 1, 0)] * (i + 1 < count) + [(i, 1)]
    turn = {trip: v for v, trip in enumerate(trips)}

    def fetch(v):
        i, own = trips[v]
        to_x, to_y = (x + VISITS[i][0]) % RING, (y + VISITS[i][1]) % RING
        to_core = core if own else 1 - core
        first = ((to_x * 2 + to_y // 2) * 2 + to_core) * 8 + to_y % 2 * RING
        start = pl.multiple_of(first * HD, 2 * BLK)
        slot = v % AHEAD
        return pltpu.make_async_copy(rows_ref.at[:, pl.ds(start, span)], columns.at[slot], sem_in.at[slot])

    for v in range(AHEAD):
        fetch(v).start()
    for k in range(wide.shape[0] // (2 * BLK)):
        power = weights_ref[pl.ds(2 * BLK * k, 2 * BLK)].reshape(1, 2 * BLK)
        weight = jnp.where(power % 2 == 1, 2.0, 1.0) * jnp.where(power >= 2, 4.0, 1.0)
        block = jnp.broadcast_to(weight, (2 * BLK, 2 * BLK)).T.astype(wide.dtype)
        for j in range(3):
            wide[2 * BLK * k : 2 * BLK * (k + 1), 2 * BLK * j : 2 * BLK * (j + 1)] = block

    def multiply(v, out):
        for i in range(RING // 2):
            even = (2 * i + RING - z) % RING
            store_pair(columns[v % AHEAD, :, 2 * i * HD : 2 * (i + 1) * HD], wide[...], out, even, (even + 1) % RING)

    def exchange(i):
        return remote(sent.at[i], got.at[i], sem_core.at[0, i], sem_core.at[1, i], partner)

    def add(i):
        a, b = VISITS[i]
        acc[a, b] = mine[i % 2] + got[i]

    events = []
    links = {}

    def message(copy, stage, d, rank, key, pieces=1):
        links[key] = (copy, (ORDERS[stage.part][stage.level], d), stage.size // pieces, rank)
        return key

    def plan(name, needs, arrivals, work, sends):
        events.append((name, needs, arrivals, work, sends))

    for i, spot in enumerate(VISITS):
        sends = []
        for s in stages[0]:
            slot = s.slot(spot)
            if s.block(spot) in (2, None):
                sends.append(message(s.far_copy(slot), s, s.parity(slot), 0, (s, "far", slot)))
            side = 1 - s.parity(slot)
            if s.block(spot) in ((1, 3)[side], None):
                sends.append(message(s.near_copy(side, slot), s, side, 2, (s, "near", side, slot)))
        plan(spot, [], [i], functools.partial(add, i), sends)
    for s, t, u in zip(*stages):
        for slot in range(s.near.shape[1]):
            d = s.parity(slot)
            send = message(s.near_copy(d, slot), s, d, 1, (s, "near", d, slot))
            plan((s, "relay", slot), [s.visit((1, 3)[d], slot)], [(s, "far", slot)], functools.partial(s.relay, slot), [send])
        for group in FAR_FIRST:
            slots = s.members(group)
            arrivals = [(s, "near", d, slot) for d in (0, 1) for slot in slots]
            sends = []
            if group == 2:
                sends = [message(t.far_copy(d), t, d, 0, (t, "far", d)) for d in (0, 1)]
            elif group:
                sends = [message(t.direct_copy(group // 2), t, group // 2, 2, (t, "direct", group // 2))]
            plan((s, group), [s.visit(0, slot) for slot in slots], arrivals, functools.partial(s.settle, group), sends)
        for before, now, after in ((s, t, u), (t, u, None)):
            for d in (0, 1):
                sends = [message(now.near_copy(d, g), now, d, 1, (now, "near", d, g), len(now.groups())) for g in now.groups()]
                plan((now, "relay", d), [(before, (1, 3)[d])], [(now, "far", d)], functools.partial(now.relay, d), sends)
            for g in now.groups():
                arrivals = [(now, kind, d, g) for d in (0, 1) for kind in ("near",)] + [(now, "direct", d) for d in (0, 1)]
                sends = []
                if after and g == 2:
                    sends = [message(after.far_copy(d), after, d, 0, (after, "far", d)) for d in (0, 1)]
                elif after and g:
                    sends = [message(after.direct_copy(g // 2), after, g // 2, 2, (after, "direct", g // 2))]
                plan((now, g), [(before, 0)], arrivals, functools.partial(now.settle, g), sends)

    done, waited, due, free = set(), set(), {}, {}
    pending = list(events)
    clock = 0.0
    r = -1
    while pending:
        now = [turn[trip] for trip in ((r + 1, 0), (r, 1)) if trip in turn]
        ready = []
        for event in list(pending):
            name, needs, arrivals, _, _ = event
            if isinstance(arrivals[0], int):
                fit = arrivals[0] == r - 1
            else:
                fit = all(n in done for n in needs) and all(due.get(m, 1e9) <= clock for m in arrivals)
            if fit:
                ready.append(event)
                pending.remove(event)
                done.add(name)
        for v in now:
            fetch(v).wait()
        for _, _, arrivals, _, _ in ready:
            for m in arrivals:
                if m not in waited:
                    waited.add(m)
                    (exchange(m) if isinstance(m, int) else links[m][0]).wait_recv()
        for v in now:
            i, own = trips[v]
            multiply(v, mine.at[i % 2] if own else sent.at[i])
        for _, _, _, work, _ in ready:
            work()
        if r == -1:
            greet([partner] + [to for stage in stages[0] for to in stage.to])
        if r + 1 < count:
            exchange(r + 1).start()
        for v in now:
            if v + AHEAD < len(trips):
                fetch(v + AHEAD).start()
        clock += VISIT_US if r <= count else TAIL_US
        for m in sorted((m for event in ready for m in event[4]), key=lambda m: links[m][3]):
            copy, link, size, _ = links[m]
            copy.start()
            free[link] = max(free.get(link, 0.0), clock) + size / LINK_RATE + 0.08
            due[m] = free[link] + HOP_US
        r += 1
    out_ref[0] = acc[0, 0, 0]
    for i in range(count):
        exchange(i).wait_send()
    for level in stages:
        for stage in level:
            stage.finish()


def gram_sums(projected, weights):
    tokens, width = projected.shape
    rows, lanes = HD, 2 * BLK
    f32 = jnp.float32
    rings = []
    for level in range(3):
        for part in range(3):
            if level:
                free = ORDERS[part][level + 1 :]
                far = (2,) + tuple(RING if a in free else 1 for a in range(3)) + (HALF, lanes)
                near = far[:-2] + (BLK, lanes)
                sems = (2,), (2, RING + 1), (3, 2)
            else:
                slots, each = ((RING, RING), (RING, RING), (RING * RING, 1))[part]
                far = (slots, each, BLK, lanes)
                near = (2,) + far
                sems = (slots,), (2, slots), (3,)
            rings += [pltpu.VMEM(far, f32), pltpu.VMEM(near, f32), *map(pltpu.SemaphoreType.DMA, sems)]
    return pl.pallas_call(
        scatter_kernel,
        in_specs=[pl.BlockSpec(memory_space=pl.ANY), pl.BlockSpec(memory_space=pltpu.VMEM)],
        out_specs=pl.BlockSpec(memory_space=pltpu.VMEM),
        out_shape=jax.ShapeDtypeStruct((1, rows, lanes), f32),
        scratch_shapes=[
            pltpu.VMEM((RING, RING, RING, rows, lanes), f32),
            pltpu.VMEM((len(VISITS), RING, rows, lanes), f32),
            pltpu.VMEM((len(VISITS), RING, rows, lanes), f32),
            pltpu.VMEM((2, RING, rows, lanes), f32),
            pltpu.VMEM((tokens, 2 * HD), projected.dtype),
            pltpu.VMEM((AHEAD, tokens, RING * HD), projected.dtype),
            *rings,
            pltpu.SemaphoreType.DMA((AHEAD,)),
            pltpu.SemaphoreType.DMA((2, len(VISITS))),
        ],
        compiler_params=pltpu.CompilerParams(collective_id=0, has_side_effects=True, vmem_limit_bytes=60 << 20),
    )(projected, weights)


def fold(block):
    return jnp.concatenate((block[:HALF], block[HALF:]), axis=1)


def whiten_kernel(total, damp_ref, packed_ref, out_ref, sems):
    head, dp = lax.axis_index("head"), lax.axis_index("dp")
    n_dp = out_ref.shape[0]
    peers = [lax.rem(dp + o, n_dp) for o in range(1, n_dp)]
    two, early = 2 * BLK, HD // 2

    def share(part):
        rows = out_ref.at[dp, pl.ds(part * early, early)]
        return [remote(rows, rows, sems.at[0, part, o], sems.at[1, part, o], {"dp": peer}) for o, peer in enumerate(peers)]

    greet([{"dp": peer} for peer in peers])
    got = packed_ref[0] / total
    even = dp % 2 == 0
    a11, a22, a33, low, a32 = (jnp.where(even, a, b) for a, b in zip(unpack_even(got), unpack_odd(got)))
    diag = lax.broadcasted_iota(jnp.int32, (BLK, BLK), 0) == lax.broadcasted_iota(jnp.int32, (BLK, BLK), 1)
    trace = jnp.sum(jnp.where(diag, a11 + a22 + a33, 0.0), axis=(0, 1), keepdims=True)
    level = trace / HD + 1e-06
    power = damp_ref[head * n_dp + dp]
    damp = jnp.where(power % 2 == 1, 0.5, 1.0) * jnp.where(power >= 2, 0.25, 1.0)
    shift = jnp.where(diag, damp * level, 0.0)
    w11 = inverse_factor(a11 + shift)
    l1 = dot_t(low, w11)
    square = dot_t(l1, l1)
    below = dot(l1, w11)
    w22 = inverse_factor(a22 + shift - square[:BLK, :BLK])
    w21 = -dot(w22, below[:BLK])
    out_ref[dp, :BLK] = jnp.concatenate((w11, w22), axis=1)
    out_ref[dp, BLK:early] = fold(w21)
    for copy in share(0):
        copy.start()
    l32 = dot_t(a32 - square[BLK:, :BLK], w22)
    w33 = inverse_factor(a33 + shift - square[BLK:, BLK:] - dot_t(l32, l32))
    w31 = -dot(w33, below[BLK:] + dot(l32, w21))
    w32 = -dot(w33, dot(l32, w22))
    out_ref[dp, early:two] = fold(w33)
    out_ref[dp, two:] = jnp.concatenate((w31, w32), axis=1)
    for copy in share(1):
        copy.start()
    for part in (0, 1):
        for copy in share(part):
            copy.wait()


def whiten(packed, damp_exp, total, n_dp):
    return pl.pallas_call(
        functools.partial(whiten_kernel, total),
        in_specs=[pl.BlockSpec(memory_space=pltpu.SMEM), pl.BlockSpec(memory_space=pltpu.VMEM)],
        out_specs=pl.BlockSpec(memory_space=pltpu.VMEM),
        out_shape=jax.ShapeDtypeStruct((n_dp,) + packed.shape[1:], jnp.float32),
        scratch_shapes=[pltpu.SemaphoreType.DMA((2, 2, n_dp - 1))],
        compiler_params=pltpu.CompilerParams(collective_id=1, has_side_effects=True),
    )(damp_exp, packed)


def unpack_kernel(packed_ref, out_ref, whole, sems):
    two, early = 2 * BLK, HD // 2
    copies = []
    for m in range(packed_ref.shape[0]):
        whole[m, :BLK, :BLK] = packed_ref[m, :BLK, :BLK]
        whole[m, :BLK, BLK:] = jnp.zeros((BLK, two), jnp.float32)
        side = packed_ref[m, BLK:early]
        below = jnp.concatenate((side[:, :BLK], side[:, BLK:]), axis=0)
        right = lax.broadcasted_iota(jnp.int32, (BLK, two), 1) >= BLK
        whole[m, BLK:two, :two] = jnp.where(right, packed_ref[m, :BLK], jnp.concatenate((below, below), axis=1))
        whole[m, BLK:two, two:] = jnp.zeros((BLK, BLK), jnp.float32)
        whole[m, two:, :two] = packed_ref[m, two:]
        last = packed_ref[m, early:two]
        whole[m, two:, two:] = jnp.concatenate((last[:, :BLK], last[:, BLK:]), axis=0)
        copy = pltpu.make_async_copy(whole.at[m], out_ref.at[m], sems.at[m])
        copy.start()
        copies.append(copy)
    for copy in copies:
        copy.wait()


def unpack(packed):
    shape = (packed.shape[0], HD, HD)
    return pl.pallas_call(
        unpack_kernel,
        in_specs=[pl.BlockSpec(memory_space=pltpu.VMEM)],
        out_specs=pl.BlockSpec(memory_space=pl.ANY),
        out_shape=jax.ShapeDtypeStruct(shape, jnp.float32),
        scratch_shapes=[pltpu.VMEM(shape, jnp.float32), pltpu.SemaphoreType.DMA(shape[:1])],
    )(packed)


def on_device(projected, weight_exp, damp_exp):
    n_dp = lax.axis_size("dp")
    total = projected.shape[0] * lax.axis_size("head") * n_dp
    owned = gram_sums(projected, weight_exp)
    return unpack(whiten(owned, damp_exp, float(total), n_dp))


def solution(mesh):
    return jax.shard_map(
        on_device,
        mesh=mesh,
        in_specs=(P(("dp", "head"), None), P(("dp", "head")), P()),
        out_specs=P("head", None, None),
        check_vma=False,
    )
```

```python
import functools

import jax
import jax.numpy as jnp
from jax import lax
from jax.experimental import pallas as pl
from jax.experimental.pallas import tpu as pltpu
from jax.sharding import PartitionSpec as P

HD = 192
BLK = HD // 3
HIGH = lax.Precision.HIGHEST


def store_pair(rows, wide, out, at, after):
    weighted = rows * wide
    contract = (((0,), (0,)), ((), ()))
    width = 4 * BLK
    first = lax.dot_general(rows[:, :width], weighted[:, :width], contract, preferred_element_type=jnp.float32)
    second = lax.dot_general(rows[:, -width:], weighted[:, -width:], contract, preferred_element_type=jnp.float32)
    two = 2 * BLK
    lanes = lax.broadcasted_iota(jnp.int32, (BLK, two), 1)
    corner = pltpu.roll(first[two : two + BLK, two:], BLK, 1)
    out[at, :BLK, :] = jnp.where(lanes < BLK, first[:BLK, :two], corner)
    out[at, BLK:, :] = first[BLK:HD, :two]
    out[after, :two, :] = second[BLK : BLK + two, two:]
    corner = pltpu.roll(second[BLK:two, :two], BLK, 1)
    out[after, two:, :] = jnp.where(lanes < BLK, corner, second[HD:, two:])


def dot(a, b):
    return lax.dot_general(a, b, (((1,), (0,)), ((), ())), precision=HIGH, preferred_element_type=jnp.float32)


def dot_t(a, b):
    return lax.dot_general(a, b, (((1,), (1,)), ((), ())), precision=HIGH, preferred_element_type=jnp.float32)


PANEL = 8


def inverse_factor(block):
    lane = lax.broadcasted_iota(jnp.int32, (PANEL, BLK), 1)
    sub = lax.broadcasted_iota(jnp.int32, (PANEL, BLK), 0)
    groups = BLK // PANEL
    each = range(PANEL)
    whole = (PANEL, BLK)
    parts = [block[PANEL * g : PANEL * g + PANEL] for g in range(groups)]

    def spread(part, at):
        return [jnp.broadcast_to(part[:, at + j : at + j + 1], whole) for j in each]

    def total(terms):
        while len(terms) > 1:
            terms = [a + b for a, b in zip(terms[::2], terms[1::2])]
        return terms[0]

    own = spread(parts[0], 0)
    for p in range(groups):
        first = PANEL * p
        columns = {g: spread(parts[g], first) for g in range(p + 1, groups)}
        ahead = spread(parts[p + 1], first + PANEL) if p + 1 < groups else None
        low = [[jnp.broadcast_to(own[j][i : i + 1], whole) for j in range(i + 1)] for i in each]
        inside = (lane >= first) & (lane < first + PANEL)
        rows = [
            jnp.where(inside, jnp.where(lane == first + i, 1.0, 0.0), jnp.broadcast_to(parts[p][i : i + 1], whole)) for i in each
        ]
        scale = []
        for k in each:
            inverse = 1.0 / low[k][k]
            scale.append(inverse)
            raw = {i: low[i][k] for i in range(k, PANEL)}
            for i in range(k + 1, PANEL):
                ratio = raw[i] * inverse
                for j in range(k + 1, i + 1):
                    low[i][j] = low[i][j] - ratio * raw[j]
                rows[i] = rows[i] - ratio * rows[k]
                low[i][k] = ratio
        done = jnp.zeros(whole, jnp.float32)
        for i in each:
            done = jnp.where((sub == i) & (lane <= first + i), rows[i] * lax.rsqrt(low[i][i]), done)
        if p + 1 < groups:
            cross = columns[p + 1]
            lifted = []
            for k in each:
                value = cross[k]
                for j in range(k):
                    value = value - low[k][j] * lifted[j]
                lifted.append(value)
            scaled = [lifted[k] * scale[k] for k in each]
            own = [
                ahead[j] - total([scaled[k] * jnp.broadcast_to(lifted[k][j : j + 1], whole) for k in each]) for j in each
            ]
            solved = [None] * PANEL
            for k in reversed(each):
                value = rows[k] * scale[k]
                for i in range(k + 1, PANEL):
                    value = value - low[i][k] * solved[i]
                solved[k] = value
            for g in range(p + 1, groups):
                parts[g] = jnp.where(inside, 0.0, parts[g]) - total([columns[g][j] * solved[j] for j in each])
        parts[p] = done
    return jnp.concatenate(parts, axis=0)


def unpack_even(got):
    two = 2 * BLK
    return got[:BLK, :BLK], got[BLK:two, BLK:], got[:BLK, BLK:], got[BLK:, :BLK], got[two:, BLK:]


def unpack_odd(got):
    two = 2 * BLK
    return got[two:, :BLK], got[BLK:two, :BLK], got[two:, BLK:], got[:BLK, :].T, got[BLK:two, BLK:].T


def remote(src, dst, send, recv, device):
    return pltpu.make_async_remote_copy(
        src_ref=src, dst_ref=dst, send_sem=send, recv_sem=recv, device_id=device, device_id_type=pl.DeviceIdType.MESH
    )


def greet(devices):
    barrier = pltpu.get_barrier_semaphore()
    for device in devices:
        pl.semaphore_signal(barrier, inc=1, device_id=device, device_id_type=pl.DeviceIdType.MESH)
    return functools.partial(pl.semaphore_wait, barrier, len(devices))


RING = 4
HALF = BLK // 2
FAR_FIRST = (2, 1, 3, 0)
ORDERS = ((0, 1, 2), (1, 2, 0), (2, 0, 1))
AHEAD = 6
VISIT_US = 1.0
TAIL_US = 0.2
HOP_US = 2.5
LINK_RATE = 46.6e3
VISITS = ((3, 2), (2, 2), (2, 3), (0, 2), (2, 1), (1, 2), (1, 1), (2, 0), (3, 3), (1, 3), (3, 1), (0, 3), (3, 0), (0, 1), (0, 0), (1, 0))


def place():
    head = lax.axis_index("head")
    dp = lax.axis_index("dp")
    return head // 4, head // 2 % 2 * 2 + dp // RING, dp % RING, head % 2


def neighbour(axis, step):
    spot = list(place())
    spot[axis] = (spot[axis] + step) % RING
    x, y, z, core = spot
    return {"head": (x * 2 + y // 2) * 2 + core, "dp": y % 2 * RING + z}


class First:
    def __init__(self, part, acc, far, near, sem_far, sem_near, sem_send):
        self.part, self.level, self.acc, self.far, self.near = part, 0, acc, far, near
        self.size = far.shape[1] * BLK * 2 * BLK * 4
        self.sem_far, self.sem_near, self.sem_send = sem_far, sem_near, sem_send
        self.to = [neighbour(part, 1), neighbour(part, -1)]
        self.rows = pl.ds(part * BLK, BLK)

    def parity(self, slot):
        return (slot + slot // RING) % 2

    def visit(self, block, slot):
        return ((block, slot), (slot, block), (slot // RING, slot % RING))[self.part]

    def slot(self, visit):
        a, b = visit
        return (b, a, RING * a + b)[self.part]

    def block(self, visit):
        return (visit[0], visit[1], None)[self.part]

    def at(self, block, slot):
        return self.visit(block, slot) + (pl.ds(block, 1) if self.part == 2 else pl.ds(0, RING), self.rows)

    def whole(self, block):
        spot = [pl.ds(0, RING)] * 3
        spot[self.part] = pl.ds(block, 1)
        return self.acc.at[tuple(spot) + (self.rows,)]

    def far_copy(self, slot):
        return remote(
            self.acc.at[self.at(2, slot)], self.far.at[slot], self.sem_send.at[0], self.sem_far.at[slot], self.to[self.parity(slot)]
        )

    def near_copy(self, d, slot):
        return remote(
            self.acc.at[self.at((1, 3)[d], slot)], self.near.at[d, slot], self.sem_send.at[1 + d], self.sem_near.at[d, slot], self.to[d]
        )

    def relay(self, slot):
        self.acc[self.at((1, 3)[self.parity(slot)], slot)] += self.far[slot]

    def members(self, group):
        return ([group], list(range(RING)), [RING * group + b for b in range(RING)])[self.part]

    def settle(self, group):
        for slot in self.members(group):
            if self.part == 1:
                self.acc[slot, 0, group, self.rows] += self.near[0, slot, group] + self.near[1, slot, group]
            else:
                self.acc[self.at(0, slot)] += self.near[0, slot] + self.near[1, slot]

    def finish(self):
        for sem, block in enumerate((2, 1, 3)):
            whole = self.whole(block)
            remote(whole, whole, self.sem_send.at[sem], self.sem_far.at[0], self.to[0]).wait_send()


class Later:
    def __init__(self, part, level, acc, far, near, sem_far, sem_near, sem_send):
        self.part, self.level, self.acc, self.far, self.near = part, level, acc, far, near
        self.size = (1 if level == 2 else RING) * HALF * 2 * BLK * 4
        self.sem_far, self.sem_near, self.sem_send = sem_far, sem_near, sem_send
        self.axis = ORDERS[part][level]
        self.free = ORDERS[part][level + 1 :]
        self.to = [neighbour(self.axis, 1), neighbour(self.axis, -1)]

    def pick(self, block, group):
        spot = [pl.ds(0, 1)] * 3
        for axis in self.free:
            spot[axis] = pl.ds(0, RING) if group is None else pl.ds(group, 1)
        spot[self.axis] = pl.ds(block, 1)
        return tuple(spot)

    def rows(self, half):
        return (pl.ds(self.part * BLK + half * HALF, HALF),)

    def copy(self, src, dst, send, recv, d):
        return remote(self.acc.at[src], dst, self.sem_send.at[send, d], recv, self.to[d])

    def far_copy(self, d):
        return self.copy(self.pick(2, None) + self.rows(d), self.far.at[(d,) + self.pick(0, None)], 0, self.sem_far.at[d], d)

    def direct_copy(self, d):
        half = self.near.at[(d,) + self.pick(0, None) + (pl.ds((1 - d) * HALF, HALF),)]
        return self.copy(self.pick((1, 3)[d], None) + self.rows(1 - d), half, 1, self.sem_near.at[d, RING], d)

    def near_copy(self, d, group):
        half = self.near.at[(d,) + self.pick(0, group) + (pl.ds(d * HALF, HALF),)]
        return self.copy(self.pick((1, 3)[d], group) + self.rows(d), half, 2, self.sem_near.at[d, group or 0], d)

    def groups(self):
        return FAR_FIRST if self.free else (0,)

    def relay(self, d):
        self.acc[self.pick((1, 3)[d], None) + self.rows(d)] += self.far[(d,) + self.pick(0, None)]

    def settle(self, group):
        spot = self.pick(0, group)
        self.acc[spot + (pl.ds(self.part * BLK, BLK),)] += self.near[(0,) + spot] + self.near[(1,) + spot]

    def finish(self):
        for d in (0, 1):
            for copy in (self.far_copy(d), self.direct_copy(d), self.near_copy(d, None)):
                copy.wait_send()


class Last:
    def __init__(self, part, acc, near, sem_near, sem_send):
        self.part, self.level, self.acc, self.near, self.sem_near, self.sem_send = part, 2, acc, near, sem_near, sem_send
        self.axis = ORDERS[part][2]
        self.rows = pl.ds(part * BLK, BLK)
        self.size = BLK * 2 * BLK * 4

    def copy(self, block):
        spot = [0, 0, 0]
        spot[self.axis] = block
        return remote(
            self.acc.at[tuple(spot) + (self.rows,)],
            self.near.at[block - 1],
            self.sem_send.at[block - 1],
            self.sem_near.at[block - 1],
            neighbour(self.axis, block),
        )

    def settle(self):
        self.acc[0, 0, 0, self.rows] += self.near[0] + self.near[1] + self.near[2]

    def finish(self):
        for block in (1, 2, 3):
            self.copy(block).wait_send()


def scatter_kernel(rows_ref, weights_ref, out_ref, acc, sent, got, mine, wide, columns, *rest):
    x, y, z, core = place()
    sem_in, sem_core = rest[-2:]
    stages = [
        [First(part, acc, *rest[5 * part :][:5]) for part in range(3)],
        [Later(part, 1, acc, *rest[15 + 5 * part :][:5]) for part in range(3)],
        [Last(part, acc, *rest[30 + 3 * part :][:3]) for part in range(3)],
    ]
    span = RING * HD
    partner = {"head": lax.axis_index("head") // 2 * 2 + 1 - core}
    count = len(VISITS)
    trips = [(0, 0)]
    for i in range(count):
        trips += [(i + 1, 0)] * (i + 1 < count) + [(i, 1)]
    turn = {trip: v for v, trip in enumerate(trips)}

    def fetch(v):
        i, own = trips[v]
        to_x, to_y = (x + VISITS[i][0]) % RING, (y + VISITS[i][1]) % RING
        to_core = core if own else 1 - core
        first = ((to_x * 2 + to_y // 2) * 2 + to_core) * 8 + to_y % 2 * RING
        start = pl.multiple_of(first * HD, 2 * BLK)
        slot = v % AHEAD
        return pltpu.make_async_copy(rows_ref.at[:, pl.ds(start, span)], columns.at[slot], sem_in.at[slot])

    met = greet([partner] + [to for stage in stages[0] for to in stage.to] + [neighbour(axis, 2) for axis in range(3)])
    for v in range(AHEAD):
        fetch(v).start()
    for k in range(wide.shape[0] // (2 * BLK)):
        power = weights_ref[pl.ds(2 * BLK * k, 2 * BLK)].reshape(1, 2 * BLK)
        weight = jnp.where(power % 2 == 1, 2.0, 1.0) * jnp.where(power >= 2, 4.0, 1.0)
        block = jnp.broadcast_to(weight, (2 * BLK, 2 * BLK)).T.astype(wide.dtype)
        for j in range(3):
            wide[2 * BLK * k : 2 * BLK * (k + 1), 2 * BLK * j : 2 * BLK * (j + 1)] = block

    def multiply(v, out):
        for i in range(RING // 2):
            even = (2 * i + RING - z) % RING
            store_pair(columns[v % AHEAD, :, 2 * i * HD : 2 * (i + 1) * HD], wide[...], out, even, (even + 1) % RING)

    def exchange(i):
        return remote(sent.at[i], got.at[i], sem_core.at[0, i], sem_core.at[1, i], partner)

    def add(i):
        a, b = VISITS[i]
        acc[a, b] = mine[i % 2] + got[i]

    events = []
    links = {}

    def message(copy, stage, d, rank, key, pieces=1):
        links[key] = (copy, (ORDERS[stage.part][stage.level], d), stage.size // pieces, rank)
        return key

    def plan(name, needs, arrivals, work, sends):
        events.append((name, needs, arrivals, work, sends))

    for i, spot in enumerate(VISITS):
        sends = []
        for s in stages[0]:
            slot = s.slot(spot)
            if s.block(spot) in (2, None):
                sends.append(message(s.far_copy(slot), s, s.parity(slot), 0, (s, "far", slot)))
            side = 1 - s.parity(slot)
            if s.block(spot) in ((1, 3)[side], None):
                sends.append(message(s.near_copy(side, slot), s, side, 2, (s, "near", side, slot)))
        plan(spot, [], [i], functools.partial(add, i), sends)
    for s, t, u in zip(*stages):
        for slot in range(s.near.shape[1]):
            d = s.parity(slot)
            send = message(s.near_copy(d, slot), s, d, 1, (s, "near", d, slot))
            plan((s, "relay", slot), [s.visit((1, 3)[d], slot)], [(s, "far", slot)], functools.partial(s.relay, slot), [send])
        for group in FAR_FIRST:
            slots = s.members(group)
            arrivals = [(s, "near", d, slot) for d in (0, 1) for slot in slots]
            sends = []
            if group == 2:
                sends = [message(t.far_copy(d), t, d, 0, (t, "far", d)) for d in (0, 1)]
            elif group:
                sends = [message(t.direct_copy(group // 2), t, group // 2, 2, (t, "direct", group // 2))]
            plan((s, group), [s.visit(0, slot) for slot in slots], arrivals, functools.partial(s.settle, group), sends)
        for d in (0, 1):
            sends = [message(t.near_copy(d, g), t, d, 1, (t, "near", d, g), RING) for g in FAR_FIRST]
            plan((t, "relay", d), [(s, (1, 3)[d])], [(t, "far", d)], functools.partial(t.relay, d), sends)
        for g in FAR_FIRST:
            arrivals = [(t, "near", d, g) for d in (0, 1)] + [(t, "direct", d) for d in (0, 1)]
            sends = [message(u.copy(g), u, g // 3, 0, (u, g))] if g else []
            plan((t, g), [(s, 0)], arrivals, functools.partial(t.settle, g), sends)
        plan((u, 0), [(t, 0)], [(u, block) for block in (1, 2, 3)], u.settle, [])

    done, waited, due, free = set(), set(), {}, {}
    pending = list(events)
    clock = 0.0
    r = -1
    while pending:
        now = [turn[trip] for trip in ((r + 1, 0), (r, 1)) if trip in turn]
        ready = []
        for event in list(pending):
            name, needs, arrivals, _, _ = event
            if isinstance(arrivals[0], int):
                fit = arrivals[0] == r - 1
            else:
                fit = all(n in done for n in needs) and all(due.get(m, 1e9) <= clock for m in arrivals)
            if fit:
                ready.append(event)
                pending.remove(event)
                done.add(name)
        for v in now:
            fetch(v).wait()
        for _, _, arrivals, _, _ in ready:
            for m in arrivals:
                if m not in waited:
                    waited.add(m)
                    (exchange(m) if isinstance(m, int) else links[m][0]).wait_recv()
        for v in now:
            i, own = trips[v]
            multiply(v, mine.at[i % 2] if own else sent.at[i])
        for _, _, _, work, _ in ready:
            work()
        if r == -1:
            met()
        if r + 1 < count:
            exchange(r + 1).start()
        for v in now:
            if v + AHEAD < len(trips):
                fetch(v + AHEAD).start()
        clock += VISIT_US if r <= count else TAIL_US
        for m in sorted((m for event in ready for m in event[4]), key=lambda m: links[m][3]):
            copy, link, size, _ = links[m]
            copy.start()
            free[link] = max(free.get(link, 0.0), clock) + size / LINK_RATE + 0.08
            due[m] = free[link] + HOP_US
        r += 1
    out_ref[0] = acc[0, 0, 0]
    for i in range(count):
        exchange(i).wait_send()
    for level in stages:
        for stage in level:
            stage.finish()


def gram_sums(projected, weights):
    tokens, width = projected.shape
    rows, lanes = HD, 2 * BLK
    f32 = jnp.float32
    rings = []
    for level in range(3):
        for part in range(3):
            if level:
                free = ORDERS[part][level + 1 :]
                far = (2,) + tuple(RING if a in free else 1 for a in range(3)) + (HALF, lanes)
                near = far[:-2] + (BLK, lanes)
                sems = (2,), (2, RING + 1), (3, 2)
                if level == 2:
                    rings += [pltpu.VMEM((3, BLK, lanes), f32), *map(pltpu.SemaphoreType.DMA, ((3,), (3,)))]
                    continue
            else:
                slots, each = ((RING, RING), (RING, RING), (RING * RING, 1))[part]
                far = (slots, each, BLK, lanes)
                near = (2,) + far
                sems = (slots,), (2, slots), (3,)
            rings += [pltpu.VMEM(far, f32), pltpu.VMEM(near, f32), *map(pltpu.SemaphoreType.DMA, sems)]
    return pl.pallas_call(
        scatter_kernel,
        in_specs=[pl.BlockSpec(memory_space=pl.ANY), pl.BlockSpec(memory_space=pltpu.VMEM)],
        out_specs=pl.BlockSpec(memory_space=pltpu.VMEM),
        out_shape=jax.ShapeDtypeStruct((1, rows, lanes), f32),
        scratch_shapes=[
            pltpu.VMEM((RING, RING, RING, rows, lanes), f32),
            pltpu.VMEM((len(VISITS), RING, rows, lanes), f32),
            pltpu.VMEM((len(VISITS), RING, rows, lanes), f32),
            pltpu.VMEM((2, RING, rows, lanes), f32),
            pltpu.VMEM((tokens, 2 * HD), projected.dtype),
            pltpu.VMEM((AHEAD, tokens, RING * HD), projected.dtype),
            *rings,
            pltpu.SemaphoreType.DMA((AHEAD,)),
            pltpu.SemaphoreType.DMA((2, len(VISITS))),
        ],
        compiler_params=pltpu.CompilerParams(collective_id=0, has_side_effects=True, vmem_limit_bytes=60 << 20),
    )(projected, weights)


def fold(block):
    return jnp.concatenate((block[:HALF], block[HALF:]), axis=1)


def whiten_kernel(total, damp_ref, packed_ref, out_ref, sems):
    head, dp = lax.axis_index("head"), lax.axis_index("dp")
    n_dp = out_ref.shape[0]
    peers = [lax.rem(dp + o, n_dp) for o in range(1, n_dp)]
    two, early = 2 * BLK, HD // 2

    def share(part):
        rows = out_ref.at[dp, pl.ds(part * early, early)]
        return [remote(rows, rows, sems.at[0, part, o], sems.at[1, part, o], {"dp": peer}) for o, peer in enumerate(peers)]

    met = greet([{"dp": peer} for peer in peers])
    got = packed_ref[0] / total
    even = dp % 2 == 0
    a11, a22, a33, low, a32 = (jnp.where(even, a, b) for a, b in zip(unpack_even(got), unpack_odd(got)))
    diag = lax.broadcasted_iota(jnp.int32, (BLK, BLK), 0) == lax.broadcasted_iota(jnp.int32, (BLK, BLK), 1)
    trace = jnp.sum(jnp.where(diag, a11 + a22 + a33, 0.0), axis=(0, 1), keepdims=True)
    level = trace / HD + 1e-06
    power = damp_ref[head * n_dp + dp]
    damp = jnp.where(power % 2 == 1, 0.5, 1.0) * jnp.where(power >= 2, 0.25, 1.0)
    shift = jnp.where(diag, damp * level, 0.0)
    w11 = inverse_factor(a11 + shift)
    l1 = dot_t(low, w11)
    square = dot_t(l1, l1)
    below = dot(l1, w11)
    w22 = inverse_factor(a22 + shift - square[:BLK, :BLK])
    w21 = -dot(w22, below[:BLK])
    out_ref[dp, :BLK] = jnp.concatenate((w11, w22), axis=1)
    out_ref[dp, BLK:early] = fold(w21)
    met()
    for copy in share(0):
        copy.start()
    l32 = dot_t(a32 - square[BLK:, :BLK], w22)
    w33 = inverse_factor(a33 + shift - square[BLK:, BLK:] - dot_t(l32, l32))
    w31 = -dot(w33, below[BLK:] + dot(l32, w21))
    w32 = -dot(w33, dot(l32, w22))
    out_ref[dp, early:two] = fold(w33)
    out_ref[dp, two:] = jnp.concatenate((w31, w32), axis=1)
    for copy in share(1):
        copy.start()
    for part in (0, 1):
        for copy in share(part):
            copy.wait()


def whiten(packed, damp_exp, total, n_dp):
    return pl.pallas_call(
        functools.partial(whiten_kernel, total),
        in_specs=[pl.BlockSpec(memory_space=pltpu.SMEM), pl.BlockSpec(memory_space=pltpu.VMEM)],
        out_specs=pl.BlockSpec(memory_space=pltpu.VMEM),
        out_shape=jax.ShapeDtypeStruct((n_dp,) + packed.shape[1:], jnp.float32),
        scratch_shapes=[pltpu.SemaphoreType.DMA((2, 2, n_dp - 1))],
        compiler_params=pltpu.CompilerParams(collective_id=1, has_side_effects=True),
    )(damp_exp, packed)


def unpack_kernel(packed_ref, out_ref, whole, sems):
    two, early = 2 * BLK, HD // 2
    copies = []
    for m in range(packed_ref.shape[0]):
        whole[m, :BLK, :BLK] = packed_ref[m, :BLK, :BLK]
        whole[m, :BLK, BLK:] = jnp.zeros((BLK, two), jnp.float32)
        side = packed_ref[m, BLK:early]
        below = jnp.concatenate((side[:, :BLK], side[:, BLK:]), axis=0)
        right = lax.broadcasted_iota(jnp.int32, (BLK, two), 1) >= BLK
        whole[m, BLK:two, :two] = jnp.where(right, packed_ref[m, :BLK], jnp.concatenate((below, below), axis=1))
        whole[m, BLK:two, two:] = jnp.zeros((BLK, BLK), jnp.float32)
        whole[m, two:, :two] = packed_ref[m, two:]
        last = packed_ref[m, early:two]
        whole[m, two:, two:] = jnp.concatenate((last[:, :BLK], last[:, BLK:]), axis=0)
        copy = pltpu.make_async_copy(whole.at[m], out_ref.at[m], sems.at[m])
        copy.start()
        copies.append(copy)
    for copy in copies:
        copy.wait()


def unpack(packed):
    shape = (packed.shape[0], HD, HD)
    return pl.pallas_call(
        unpack_kernel,
        in_specs=[pl.BlockSpec(memory_space=pltpu.VMEM)],
        out_specs=pl.BlockSpec(memory_space=pl.ANY),
        out_shape=jax.ShapeDtypeStruct(shape, jnp.float32),
        scratch_shapes=[pltpu.VMEM(shape, jnp.float32), pltpu.SemaphoreType.DMA(shape[:1])],
    )(packed)


def on_device(projected, weight_exp, damp_exp):
    n_dp = lax.axis_size("dp")
    total = projected.shape[0] * lax.axis_size("head") * n_dp
    owned = gram_sums(projected, weight_exp)
    return unpack(whiten(owned, damp_exp, float(total), n_dp))


def solution(mesh):
    return jax.shard_map(
        on_device,
        mesh=mesh,
        in_specs=(P(("dp", "head"), None), P(("dp", "head")), P()),
        out_specs=P("head", None, None),
        check_vma=False,
    )
```

```python
import functools

import jax
import jax.numpy as jnp
from jax import lax
from jax.experimental import pallas as pl
from jax.experimental.pallas import tpu as pltpu
from jax.sharding import PartitionSpec as P

HD = 192
BLK = HD // 3
HIGH = lax.Precision.HIGHEST


def store_pair(rows, wide, out, at, after):
    weighted = rows * wide
    across = (((1,), (0,)), ((), ()))
    width, two = 4 * BLK, 2 * BLK
    first = lax.dot_general(rows[:, :HD], weighted[:, :width], (((0,), (0,)), ((), ())), preferred_element_type=jnp.float32)
    turned = rows[:, -width:].T[BLK:]
    second = lax.dot_general(turned, weighted[:, -width:], across, preferred_element_type=jnp.float32)
    lanes = lax.broadcasted_iota(jnp.int32, (BLK, two), 1)
    corner = pltpu.roll(first[two:, two:], BLK, 1)
    out[at, :BLK, :] = jnp.where(lanes < BLK, first[:BLK, :two], corner)
    out[at, BLK:, :] = first[BLK:HD, :two]
    out[after, :two, :] = second[:two, two:]
    corner = pltpu.roll(second[:BLK, :two], BLK, 1)
    out[after, two:, :] = jnp.where(lanes < BLK, corner, second[two:, two:])


def dot(a, b):
    return lax.dot_general(a, b, (((1,), (0,)), ((), ())), precision=HIGH, preferred_element_type=jnp.float32)


def dot_t(a, b):
    return lax.dot_general(a, b, (((1,), (1,)), ((), ())), precision=HIGH, preferred_element_type=jnp.float32)


PANEL = 8


def inverse_factor(block):
    lane = lax.broadcasted_iota(jnp.int32, (PANEL, BLK), 1)
    sub = lax.broadcasted_iota(jnp.int32, (PANEL, BLK), 0)
    groups = BLK // PANEL
    each = range(PANEL)
    whole = (PANEL, BLK)
    parts = [block[PANEL * g : PANEL * g + PANEL] for g in range(groups)]

    def spread(part, at):
        return [jnp.broadcast_to(part[:, at + j : at + j + 1], whole) for j in each]

    def total(terms):
        while len(terms) > 1:
            terms = [a + b for a, b in zip(terms[::2], terms[1::2])]
        return terms[0]

    own = spread(parts[0], 0)
    for p in range(groups):
        first = PANEL * p
        columns = {g: spread(parts[g], first) for g in range(p + 1, groups)}
        ahead = spread(parts[p + 1], first + PANEL) if p + 1 < groups else None
        low = [[jnp.broadcast_to(own[j][i : i + 1], whole) for j in range(i + 1)] for i in each]
        inside = (lane >= first) & (lane < first + PANEL)
        rows = [
            jnp.where(inside, jnp.where(lane == first + i, 1.0, 0.0), jnp.broadcast_to(parts[p][i : i + 1], whole)) for i in each
        ]
        scale = []
        for k in each:
            inverse = 1.0 / low[k][k]
            scale.append(inverse)
            raw = {i: low[i][k] for i in range(k, PANEL)}
            for i in range(k + 1, PANEL):
                ratio = raw[i] * inverse
                for j in range(k + 1, i + 1):
                    low[i][j] = low[i][j] - ratio * raw[j]
                rows[i] = rows[i] - ratio * rows[k]
                low[i][k] = ratio
        done = jnp.zeros(whole, jnp.float32)
        for i in each:
            done = jnp.where((sub == i) & (lane <= first + i), rows[i] * lax.rsqrt(low[i][i]), done)
        if p + 1 < groups:
            cross = columns[p + 1]
            lifted = []
            for k in each:
                value = cross[k]
                for j in range(k):
                    value = value - low[k][j] * lifted[j]
                lifted.append(value)
            scaled = [lifted[k] * scale[k] for k in each]
            own = [
                ahead[j] - total([scaled[k] * jnp.broadcast_to(lifted[k][j : j + 1], whole) for k in each]) for j in each
            ]
            solved = [None] * PANEL
            for k in reversed(each):
                value = rows[k] * scale[k]
                for i in range(k + 1, PANEL):
                    value = value - low[i][k] * solved[i]
                solved[k] = value
            for g in range(p + 1, groups):
                parts[g] = jnp.where(inside, 0.0, parts[g]) - total([columns[g][j] * solved[j] for j in each])
        parts[p] = done
    return jnp.concatenate(parts, axis=0)


def unpack_even(got):
    two = 2 * BLK
    return got[:BLK, :BLK], got[BLK:two, BLK:], got[:BLK, BLK:], got[BLK:, :BLK], got[two:, BLK:]


def unpack_odd(got):
    two = 2 * BLK
    return got[two:, :BLK], got[BLK:two, :BLK], got[two:, BLK:], got[:BLK, :].T, got[BLK:two, BLK:].T


def remote(src, dst, send, recv, device):
    return pltpu.make_async_remote_copy(
        src_ref=src, dst_ref=dst, send_sem=send, recv_sem=recv, device_id=device, device_id_type=pl.DeviceIdType.MESH
    )


def greet(devices):
    barrier = pltpu.get_barrier_semaphore()
    for device in devices:
        pl.semaphore_signal(barrier, inc=1, device_id=device, device_id_type=pl.DeviceIdType.MESH)
    return functools.partial(pl.semaphore_wait, barrier, len(devices))


RING = 4
HALF = BLK // 2
FAR_FIRST = (2, 1, 3, 0)
ORDERS = ((0, 1, 2), (1, 2, 0), (2, 0, 1))
AHEAD = 6
VISIT_US = 0.85
TAIL_US = 0.2
HOP_US = 2.5
LINK_RATE = 46.6e3
VISITS = ((3, 2), (2, 2), (2, 3), (0, 2), (2, 1), (1, 2), (1, 1), (2, 0), (3, 3), (1, 3), (3, 1), (0, 3), (3, 0), (0, 1), (0, 0), (1, 0))


def place():
    head = lax.axis_index("head")
    dp = lax.axis_index("dp")
    return head // 4, head // 2 % 2 * 2 + dp // RING, dp % RING, head % 2


def neighbour(axis, step):
    spot = list(place())
    spot[axis] = (spot[axis] + step) % RING
    x, y, z, core = spot
    return {"head": (x * 2 + y // 2) * 2 + core, "dp": y % 2 * RING + z}


def fold(block):
    return jnp.concatenate((block[:HALF], block[HALF:]), axis=1)


def whiten(packed, damp_ref, total, out_ref, sems):
    head, dp = lax.axis_index("head"), lax.axis_index("dp")
    n_dp = out_ref.shape[0]
    peers = [lax.rem(dp + o, n_dp) for o in range(1, n_dp)]
    two, early = 2 * BLK, HD // 2

    def share(part):
        rows = out_ref.at[dp, pl.ds(part * early, early)]
        return [remote(rows, rows, sems.at[0, part, o], sems.at[1, part, o], {"dp": peer}) for o, peer in enumerate(peers)]

    got = packed / total
    even = dp % 2 == 0
    a11, a22, a33, low, a32 = (jnp.where(even, a, b) for a, b in zip(unpack_even(got), unpack_odd(got)))
    diag = lax.broadcasted_iota(jnp.int32, (BLK, BLK), 0) == lax.broadcasted_iota(jnp.int32, (BLK, BLK), 1)
    trace = jnp.sum(jnp.where(diag, a11 + a22 + a33, 0.0), axis=(0, 1), keepdims=True)
    level = trace / HD + 1e-06
    power = damp_ref[head * n_dp + dp]
    damp = jnp.where(power % 2 == 1, 0.5, 1.0) * jnp.where(power >= 2, 0.25, 1.0)
    shift = jnp.where(diag, damp * level, 0.0)
    w11 = inverse_factor(a11 + shift)
    l1 = dot_t(low, w11)
    square = dot_t(l1, l1)
    below = dot(l1, w11)
    w22 = inverse_factor(a22 + shift - square[:BLK, :BLK])
    w21 = -dot(w22, below[:BLK])
    out_ref[dp, :BLK] = jnp.concatenate((w11, w22), axis=1)
    out_ref[dp, BLK:early] = fold(w21)
    for copy in share(0):
        copy.start()
    l32 = dot_t(a32 - square[BLK:, :BLK], w22)
    w33 = inverse_factor(a33 + shift - square[BLK:, BLK:] - dot_t(l32, l32))
    w31 = -dot(w33, below[BLK:] + dot(l32, w21))
    w32 = -dot(w33, dot(l32, w22))
    out_ref[dp, early:two] = fold(w33)
    out_ref[dp, two:] = jnp.concatenate((w31, w32), axis=1)
    for copy in share(1):
        copy.start()
    for part in (0, 1):
        for copy in share(part):
            copy.wait()


class First:
    def __init__(self, part, acc, far, near, sem_far, sem_near, sem_send):
        self.part, self.level, self.acc, self.far, self.near = part, 0, acc, far, near
        self.size = far.shape[1] * BLK * 2 * BLK * 4
        self.sem_far, self.sem_near, self.sem_send = sem_far, sem_near, sem_send
        self.to = [neighbour(part, 1), neighbour(part, -1)]
        self.rows = pl.ds(part * BLK, BLK)

    def parity(self, slot):
        return (slot + slot // RING) % 2

    def visit(self, block, slot):
        return ((block, slot), (slot, block), (slot // RING, slot % RING))[self.part]

    def slot(self, visit):
        a, b = visit
        return (b, a, RING * a + b)[self.part]

    def block(self, visit):
        return (visit[0], visit[1], None)[self.part]

    def at(self, block, slot):
        return self.visit(block, slot) + (pl.ds(block, 1) if self.part == 2 else pl.ds(0, RING), self.rows)

    def whole(self, block):
        spot = [pl.ds(0, RING)] * 3
        spot[self.part] = pl.ds(block, 1)
        return self.acc.at[tuple(spot) + (self.rows,)]

    def far_copy(self, slot):
        return remote(
            self.acc.at[self.at(2, slot)], self.far.at[slot], self.sem_send.at[0], self.sem_far.at[slot], self.to[self.parity(slot)]
        )

    def near_copy(self, d, slot):
        return remote(
            self.acc.at[self.at((1, 3)[d], slot)], self.near.at[d, slot], self.sem_send.at[1 + d], self.sem_near.at[d, slot], self.to[d]
        )

    def relay(self, slot):
        self.acc[self.at((1, 3)[self.parity(slot)], slot)] += self.far[slot]

    def members(self, group):
        return ([group], list(range(RING)), [RING * group + b for b in range(RING)])[self.part]

    def settle(self, group):
        for slot in self.members(group):
            if self.part == 1:
                self.acc[slot, 0, group, self.rows] += self.near[0, slot, group] + self.near[1, slot, group]
            else:
                self.acc[self.at(0, slot)] += self.near[0, slot] + self.near[1, slot]

    def finish(self):
        for sem, block in enumerate((2, 1, 3)):
            whole = self.whole(block)
            remote(whole, whole, self.sem_send.at[sem], self.sem_far.at[0], self.to[0]).wait_send()


class Later:
    def __init__(self, part, level, acc, far, near, sem_far, sem_near, sem_send):
        self.part, self.level, self.acc, self.far, self.near = part, level, acc, far, near
        self.size = (1 if level == 2 else RING) * HALF * 2 * BLK * 4
        self.sem_far, self.sem_near, self.sem_send = sem_far, sem_near, sem_send
        self.axis = ORDERS[part][level]
        self.free = ORDERS[part][level + 1 :]
        self.to = [neighbour(self.axis, 1), neighbour(self.axis, -1)]

    def pick(self, block, group):
        spot = [pl.ds(0, 1)] * 3
        for axis in self.free:
            spot[axis] = pl.ds(0, RING) if group is None else pl.ds(group, 1)
        spot[self.axis] = pl.ds(block, 1)
        return tuple(spot)

    def rows(self, half):
        return (pl.ds(self.part * BLK + half * HALF, HALF),)

    def copy(self, src, dst, send, recv, d):
        return remote(self.acc.at[src], dst, self.sem_send.at[send, d], recv, self.to[d])

    def far_copy(self, d):
        return self.copy(self.pick(2, None) + self.rows(d), self.far.at[(d,) + self.pick(0, None)], 0, self.sem_far.at[d], d)

    def direct_copy(self, d):
        half = self.near.at[(d,) + self.pick(0, None) + (pl.ds((1 - d) * HALF, HALF),)]
        return self.copy(self.pick((1, 3)[d], None) + self.rows(1 - d), half, 1, self.sem_near.at[d, RING], d)

    def near_copy(self, d, group):
        half = self.near.at[(d,) + self.pick(0, group) + (pl.ds(d * HALF, HALF),)]
        return self.copy(self.pick((1, 3)[d], group) + self.rows(d), half, 2, self.sem_near.at[d, group or 0], d)

    def groups(self):
        return FAR_FIRST if self.free else (0,)

    def relay(self, d):
        self.acc[self.pick((1, 3)[d], None) + self.rows(d)] += self.far[(d,) + self.pick(0, None)]

    def settle(self, group):
        spot = self.pick(0, group)
        self.acc[spot + (pl.ds(self.part * BLK, BLK),)] += self.near[(0,) + spot] + self.near[(1,) + spot]

    def finish(self):
        for d in (0, 1):
            for copy in (self.far_copy(d), self.direct_copy(d), self.near_copy(d, None)):
                copy.wait_send()


class Last:
    def __init__(self, part, acc, near, sem_near, sem_send):
        self.part, self.level, self.acc, self.near, self.sem_near, self.sem_send = part, 2, acc, near, sem_near, sem_send
        self.axis = ORDERS[part][2]
        self.rows = pl.ds(part * BLK, BLK)
        self.size = BLK * 2 * BLK * 4

    def copy(self, block):
        spot = [0, 0, 0]
        spot[self.axis] = block
        return remote(
            self.acc.at[tuple(spot) + (self.rows,)],
            self.near.at[block - 1],
            self.sem_send.at[block - 1],
            self.sem_near.at[block - 1],
            neighbour(self.axis, block),
        )

    def settle(self):
        self.acc[0, 0, 0, self.rows] += self.near[0] + self.near[1] + self.near[2]

    def finish(self):
        for block in (1, 2, 3):
            self.copy(block).wait_send()


def factor_kernel(total, rows_ref, weights_ref, damp_ref, out_ref, acc, sent, got, mine, wide, columns, *rest):
    x, y, z, core = place()
    sem_in, sem_core, sem_share = rest[-3:]
    stages = [
        [First(part, acc, *rest[5 * part :][:5]) for part in range(3)],
        [Later(part, 1, acc, *rest[15 + 5 * part :][:5]) for part in range(3)],
        [Last(part, acc, *rest[30 + 3 * part :][:3]) for part in range(3)],
    ]
    span = RING * HD
    partner = {"head": lax.axis_index("head") // 2 * 2 + 1 - core}
    count = len(VISITS)
    trips = [(0, 0)]
    for i in range(count):
        trips += [(i + 1, 0)] * (i + 1 < count) + [(i, 1)]
    turn = {trip: v for v, trip in enumerate(trips)}

    def fetch(v):
        i, own = trips[v]
        to_x, to_y = (x + VISITS[i][0]) % RING, (y + VISITS[i][1]) % RING
        to_core = core if own else 1 - core
        first = ((to_x * 2 + to_y // 2) * 2 + to_core) * 8 + to_y % 2 * RING
        start = pl.multiple_of(first * HD, 2 * BLK)
        slot = v % AHEAD
        return pltpu.make_async_copy(rows_ref.at[:, pl.ds(start, span)], columns.at[slot], sem_in.at[slot])

    n_dp = out_ref.shape[0]
    peers = [{"dp": lax.rem(lax.axis_index("dp") + o, n_dp)} for o in range(1, n_dp)]
    met = greet([partner] + [to for stage in stages[0] for to in stage.to] + [neighbour(axis, 2) for axis in range(3)] + peers)
    for v in range(AHEAD):
        fetch(v).start()
    for k in range(wide.shape[0] // (2 * BLK)):
        power = weights_ref[pl.ds(2 * BLK * k, 2 * BLK)].reshape(1, 2 * BLK)
        weight = jnp.where(power % 2 == 1, 2.0, 1.0) * jnp.where(power >= 2, 4.0, 1.0)
        block = jnp.broadcast_to(weight, (2 * BLK, 2 * BLK)).T.astype(wide.dtype)
        for j in range(3):
            wide[2 * BLK * k : 2 * BLK * (k + 1), 2 * BLK * j : 2 * BLK * (j + 1)] = block

    def multiply(v, out):
        for i in range(RING // 2):
            even = (2 * i + RING - z) % RING
            store_pair(columns[v % AHEAD, :, 2 * i * HD : 2 * (i + 1) * HD], wide[...], out, even, (even + 1) % RING)

    def exchange(i):
        return remote(sent.at[i], got.at[i], sem_core.at[0, i], sem_core.at[1, i], partner)

    def add(i):
        a, b = VISITS[i]
        acc[a, b] = mine[i % 2] + got[i]

    events = []
    links = {}

    def message(copy, stage, d, rank, key, pieces=1):
        links[key] = (copy, (ORDERS[stage.part][stage.level], d), stage.size // pieces, rank)
        return key

    def plan(name, needs, arrivals, work, sends):
        events.append((name, needs, arrivals, work, sends))

    for i, spot in enumerate(VISITS):
        sends = []
        for s in stages[0]:
            slot = s.slot(spot)
            if s.block(spot) in (2, None):
                sends.append(message(s.far_copy(slot), s, s.parity(slot), 0, (s, "far", slot)))
            side = 1 - s.parity(slot)
            if s.block(spot) in ((1, 3)[side], None):
                sends.append(message(s.near_copy(side, slot), s, side, 2, (s, "near", side, slot)))
        plan(spot, [], [i], functools.partial(add, i), sends)
    for s, t, u in zip(*stages):
        for slot in range(s.near.shape[1]):
            d = s.parity(slot)
            send = message(s.near_copy(d, slot), s, d, 1, (s, "near", d, slot))
            plan((s, "relay", slot), [s.visit((1, 3)[d], slot)], [(s, "far", slot)], functools.partial(s.relay, slot), [send])
        for group in FAR_FIRST:
            slots = s.members(group)
            arrivals = [(s, "near", d, slot) for d in (0, 1) for slot in slots]
            sends = []
            if group == 2:
                sends = [message(t.far_copy(d), t, d, 0, (t, "far", d)) for d in (0, 1)]
            elif group:
                sends = [message(t.direct_copy(group // 2), t, group // 2, 2, (t, "direct", group // 2))]
            plan((s, group), [s.visit(0, slot) for slot in slots], arrivals, functools.partial(s.settle, group), sends)
        for d in (0, 1):
            sends = [message(t.near_copy(d, g), t, d, 1, (t, "near", d, g), RING) for g in FAR_FIRST]
            plan((t, "relay", d), [(s, (1, 3)[d])], [(t, "far", d)], functools.partial(t.relay, d), sends)
        for g in FAR_FIRST:
            arrivals = [(t, "near", d, g) for d in (0, 1)] + [(t, "direct", d) for d in (0, 1)]
            sends = [message(u.copy(g), u, g // 3, 0, (u, g))] if g else []
            plan((t, g), [(s, 0)], arrivals, functools.partial(t.settle, g), sends)
        plan((u, 0), [(t, 0)], [(u, block) for block in (1, 2, 3)], u.settle, [])

    done, waited, due, free = set(), set(), {}, {}
    pending = list(events)
    clock = 0.0
    r = -1
    while pending:
        now = [turn[trip] for trip in ((r + 1, 0), (r, 1)) if trip in turn]
        ready = []
        for event in list(pending):
            name, needs, arrivals, _, _ = event
            if isinstance(arrivals[0], int):
                fit = arrivals[0] == r - 1
            else:
                fit = all(n in done for n in needs) and all(due.get(m, 1e9) <= clock for m in arrivals)
            if fit:
                ready.append(event)
                pending.remove(event)
                done.add(name)
        for v in now:
            fetch(v).wait()
        for _, _, arrivals, _, _ in ready:
            for m in arrivals:
                if m not in waited:
                    waited.add(m)
                    (exchange(m) if isinstance(m, int) else links[m][0]).wait_recv()
        for v in now:
            i, own = trips[v]
            multiply(v, mine.at[i % 2] if own else sent.at[i])
        for _, _, _, work, _ in ready:
            work()
        if r == -1:
            met()
        if r + 1 < count:
            exchange(r + 1).start()
        for v in now:
            if v + AHEAD < len(trips):
                fetch(v + AHEAD).start()
        clock += VISIT_US if r <= count else TAIL_US
        for m in sorted((m for event in ready for m in event[4]), key=lambda m: links[m][3]):
            copy, link, size, _ = links[m]
            copy.start()
            free[link] = max(free.get(link, 0.0), clock) + size / LINK_RATE + 0.08
            due[m] = free[link] + HOP_US
        r += 1
    whiten(acc[0, 0, 0], damp_ref, total, out_ref, sem_share)
    for i in range(count):
        exchange(i).wait_send()
    for level in stages:
        for stage in level:
            stage.finish()


def factors(projected, weights, damp_exp, total, n_dp):
    tokens, width = projected.shape
    rows, lanes = HD, 2 * BLK
    f32 = jnp.float32
    rings = []
    for level in range(3):
        for part in range(3):
            if level:
                free = ORDERS[part][level + 1 :]
                far = (2,) + tuple(RING if a in free else 1 for a in range(3)) + (HALF, lanes)
                near = far[:-2] + (BLK, lanes)
                sems = (2,), (2, RING + 1), (3, 2)
                if level == 2:
                    rings += [pltpu.VMEM((3, BLK, lanes), f32), *map(pltpu.SemaphoreType.DMA, ((3,), (3,)))]
                    continue
            else:
                slots, each = ((RING, RING), (RING, RING), (RING * RING, 1))[part]
                far = (slots, each, BLK, lanes)
                near = (2,) + far
                sems = (slots,), (2, slots), (3,)
            rings += [pltpu.VMEM(far, f32), pltpu.VMEM(near, f32), *map(pltpu.SemaphoreType.DMA, sems)]
    return pl.pallas_call(
        functools.partial(factor_kernel, total),
        in_specs=[
            pl.BlockSpec(memory_space=pl.ANY),
            pl.BlockSpec(memory_space=pltpu.VMEM),
            pl.BlockSpec(memory_space=pltpu.SMEM),
        ],
        out_specs=pl.BlockSpec(memory_space=pltpu.VMEM),
        out_shape=jax.ShapeDtypeStruct((n_dp, rows, lanes), f32),
        scratch_shapes=[
            pltpu.VMEM((RING, RING, RING, rows, lanes), f32),
            pltpu.VMEM((len(VISITS), RING, rows, lanes), f32),
            pltpu.VMEM((len(VISITS), RING, rows, lanes), f32),
            pltpu.VMEM((2, RING, rows, lanes), f32),
            pltpu.VMEM((tokens, 2 * HD), projected.dtype),
            pltpu.VMEM((AHEAD, tokens, RING * HD), projected.dtype),
            *rings,
            pltpu.SemaphoreType.DMA((AHEAD,)),
            pltpu.SemaphoreType.DMA((2, len(VISITS))),
            pltpu.SemaphoreType.DMA((2, 2, n_dp - 1)),
        ],
        compiler_params=pltpu.CompilerParams(collective_id=0, has_side_effects=True, vmem_limit_bytes=60 << 20),
    )(projected, weights, damp_exp)


def unpack_kernel(packed_ref, out_ref, whole, sems):
    two, early = 2 * BLK, HD // 2
    copies = []
    for m in range(packed_ref.shape[0]):
        whole[m, :BLK, :BLK] = packed_ref[m, :BLK, :BLK]
        whole[m, :BLK, BLK:] = jnp.zeros((BLK, two), jnp.float32)
        side = packed_ref[m, BLK:early]
        below = jnp.concatenate((side[:, :BLK], side[:, BLK:]), axis=0)
        right = lax.broadcasted_iota(jnp.int32, (BLK, two), 1) >= BLK
        whole[m, BLK:two, :two] = jnp.where(right, packed_ref[m, :BLK], jnp.concatenate((below, below), axis=1))
        whole[m, BLK:two, two:] = jnp.zeros((BLK, BLK), jnp.float32)
        whole[m, two:, :two] = packed_ref[m, two:]
        last = packed_ref[m, early:two]
        whole[m, two:, two:] = jnp.concatenate((last[:, :BLK], last[:, BLK:]), axis=0)
        copy = pltpu.make_async_copy(whole.at[m], out_ref.at[m], sems.at[m])
        copy.start()
        copies.append(copy)
    for copy in copies:
        copy.wait()


def unpack(packed):
    shape = (packed.shape[0], HD, HD)
    return pl.pallas_call(
        unpack_kernel,
        in_specs=[pl.BlockSpec(memory_space=pltpu.VMEM)],
        out_specs=pl.BlockSpec(memory_space=pl.ANY),
        out_shape=jax.ShapeDtypeStruct(shape, jnp.float32),
        scratch_shapes=[pltpu.VMEM(shape, jnp.float32), pltpu.SemaphoreType.DMA(shape[:1])],
    )(packed)


def on_device(projected, weight_exp, damp_exp):
    n_dp = lax.axis_size("dp")
    total = projected.shape[0] * lax.axis_size("head") * n_dp
    return unpack(factors(projected, weight_exp, damp_exp, float(total), n_dp))


def solution(mesh):
    return jax.shard_map(
        on_device,
        mesh=mesh,
        in_specs=(P(("dp", "head"), None), P(("dp", "head")), P()),
        out_specs=P("head", None, None),
        check_vma=False,
    )
```

```python
import functools

import jax
import jax.numpy as jnp
from jax import lax
from jax.experimental import pallas as pl
from jax.experimental.pallas import tpu as pltpu
from jax.sharding import PartitionSpec as P

HD = 192
BLK = HD // 3
HIGH = lax.Precision.HIGHEST


def store_pair(rows, wide, out, at, after):
    weighted = rows * wide
    across = (((1,), (0,)), ((), ()))
    width, two = 4 * BLK, 2 * BLK
    first = lax.dot_general(rows[:, :HD], weighted[:, :width], (((0,), (0,)), ((), ())), preferred_element_type=jnp.float32)
    turned = rows[:, -width:].T[BLK:]
    second = lax.dot_general(turned, weighted[:, -width:], across, preferred_element_type=jnp.float32)
    lanes = lax.broadcasted_iota(jnp.int32, (BLK, two), 1)
    corner = pltpu.roll(first[two:, two:], BLK, 1)
    out[at, :BLK, :] = jnp.where(lanes < BLK, first[:BLK, :two], corner)
    out[at, BLK:, :] = first[BLK:HD, :two]
    out[after, :two, :] = second[:two, two:]
    corner = pltpu.roll(second[:BLK, :two], BLK, 1)
    out[after, two:, :] = jnp.where(lanes < BLK, corner, second[two:, two:])


def dot(a, b):
    return lax.dot_general(a, b, (((1,), (0,)), ((), ())), precision=HIGH, preferred_element_type=jnp.float32)


def dot_t(a, b):
    return lax.dot_general(a, b, (((1,), (1,)), ((), ())), precision=HIGH, preferred_element_type=jnp.float32)


PANEL = 8


def inverse_factor(block):
    lane = lax.broadcasted_iota(jnp.int32, (PANEL, BLK), 1)
    sub = lax.broadcasted_iota(jnp.int32, (PANEL, BLK), 0)
    groups = BLK // PANEL
    each = range(PANEL)
    whole = (PANEL, BLK)
    parts = [block[PANEL * g : PANEL * g + PANEL] for g in range(groups)]

    def spread(part, at):
        return [jnp.broadcast_to(part[:, at + j : at + j + 1], whole) for j in each]

    def total(terms):
        while len(terms) > 1:
            terms = [a + b for a, b in zip(terms[::2], terms[1::2])]
        return terms[0]

    own = spread(parts[0], 0)
    for p in range(groups):
        first = PANEL * p
        columns = {g: spread(parts[g], first) for g in range(p + 1, groups)}
        ahead = spread(parts[p + 1], first + PANEL) if p + 1 < groups else None
        low = [[jnp.broadcast_to(own[j][i : i + 1], whole) for j in range(i + 1)] for i in each]
        inside = (lane >= first) & (lane < first + PANEL)
        rows = [
            jnp.where(inside, jnp.where(lane == first + i, 1.0, 0.0), jnp.broadcast_to(parts[p][i : i + 1], whole)) for i in each
        ]
        scale = []
        for k in each:
            inverse = 1.0 / low[k][k]
            scale.append(inverse)
            raw = {i: low[i][k] for i in range(k, PANEL)}
            for i in range(k + 1, PANEL):
                ratio = raw[i] * inverse
                for j in range(k + 1, i + 1):
                    low[i][j] = low[i][j] - ratio * raw[j]
                rows[i] = rows[i] - ratio * rows[k]
                low[i][k] = ratio
        done = jnp.zeros(whole, jnp.float32)
        for i in each:
            done = jnp.where((sub == i) & (lane <= first + i), rows[i] * lax.rsqrt(low[i][i]), done)
        if p + 1 < groups:
            cross = columns[p + 1]
            lifted = []
            for k in each:
                value = cross[k]
                for j in range(k):
                    value = value - low[k][j] * lifted[j]
                lifted.append(value)
            scaled = [lifted[k] * scale[k] for k in each]
            own = [
                ahead[j] - total([scaled[k] * jnp.broadcast_to(lifted[k][j : j + 1], whole) for k in each]) for j in each
            ]
            solved = [None] * PANEL
            for k in reversed(each):
                value = rows[k] * scale[k]
                for i in range(k + 1, PANEL):
                    value = value - low[i][k] * solved[i]
                solved[k] = value
            for g in range(p + 1, groups):
                parts[g] = jnp.where(inside, 0.0, parts[g]) - total([columns[g][j] * solved[j] for j in each])
        parts[p] = done
    return jnp.concatenate(parts, axis=0)


def unpack_even(got):
    two = 2 * BLK
    return got[:BLK, :BLK], got[BLK:two, BLK:], got[:BLK, BLK:], got[BLK:, :BLK], got[two:, BLK:]


def unpack_odd(got):
    two = 2 * BLK
    return got[two:, :BLK], got[BLK:two, :BLK], got[two:, BLK:], got[:BLK, :].T, got[BLK:two, BLK:].T


def remote(src, dst, send, recv, device):
    return pltpu.make_async_remote_copy(
        src_ref=src, dst_ref=dst, send_sem=send, recv_sem=recv, device_id=device, device_id_type=pl.DeviceIdType.MESH
    )


def greet(devices):
    barrier = pltpu.get_barrier_semaphore()
    for device in devices:
        pl.semaphore_signal(barrier, inc=1, device_id=device, device_id_type=pl.DeviceIdType.MESH)
    return functools.partial(pl.semaphore_wait, barrier, len(devices))


RING = 4
HALF = BLK // 2
FAR_FIRST = (2, 1, 3, 0)
ORDERS = ((0, 1, 2), (1, 2, 0), (2, 0, 1))
AHEAD = 6
VISIT_US = 0.85
TAIL_US = 0.2
HOP_US = 3.5
LINK_RATE = 46.6e3
VISITS = ((3, 2), (2, 2), (2, 3), (0, 2), (2, 1), (1, 2), (1, 1), (2, 0), (3, 3), (1, 3), (3, 1), (0, 3), (3, 0), (0, 1), (0, 0), (1, 0))


def place():
    head = lax.axis_index("head")
    dp = lax.axis_index("dp")
    return head // 4, head // 2 % 2 * 2 + dp // RING, dp % RING, head % 2


def neighbour(axis, step):
    spot = list(place())
    spot[axis] = (spot[axis] + step) % RING
    x, y, z, core = spot
    return {"head": (x * 2 + y // 2) * 2 + core, "dp": y % 2 * RING + z}


def fold(block):
    return jnp.concatenate((block[:HALF], block[HALF:]), axis=1)


def whiten(packed, damp_ref, total, out_ref, sems):
    head, dp = lax.axis_index("head"), lax.axis_index("dp")
    n_dp = out_ref.shape[0]
    peers = [lax.rem(dp + o, n_dp) for o in range(1, n_dp)]
    two, early = 2 * BLK, HD // 2

    def share(part):
        rows = out_ref.at[dp, pl.ds(part * early, early)]
        return [remote(rows, rows, sems.at[0, part, o], sems.at[1, part, o], {"dp": peer}) for o, peer in enumerate(peers)]

    got = packed / total
    even = dp % 2 == 0
    a11, a22, a33, low, a32 = (jnp.where(even, a, b) for a, b in zip(unpack_even(got), unpack_odd(got)))
    diag = lax.broadcasted_iota(jnp.int32, (BLK, BLK), 0) == lax.broadcasted_iota(jnp.int32, (BLK, BLK), 1)
    trace = jnp.sum(jnp.where(diag, a11 + a22 + a33, 0.0), axis=(0, 1), keepdims=True)
    level = trace / HD + 1e-06
    power = damp_ref[head * n_dp + dp]
    damp = jnp.where(power % 2 == 1, 0.5, 1.0) * jnp.where(power >= 2, 0.25, 1.0)
    shift = jnp.where(diag, damp * level, 0.0)
    w11 = inverse_factor(a11 + shift)
    l1 = dot_t(low, w11)
    square = dot_t(l1, l1)
    below = dot(l1, w11)
    w22 = inverse_factor(a22 + shift - square[:BLK, :BLK])
    w21 = -dot(w22, below[:BLK])
    out_ref[dp, :BLK] = jnp.concatenate((w11, w22), axis=1)
    out_ref[dp, BLK:early] = fold(w21)
    for copy in share(0):
        copy.start()
    l32 = dot_t(a32 - square[BLK:, :BLK], w22)
    w33 = inverse_factor(a33 + shift - square[BLK:, BLK:] - dot_t(l32, l32))
    w31 = -dot(w33, below[BLK:] + dot(l32, w21))
    w32 = -dot(w33, dot(l32, w22))
    out_ref[dp, early:two] = fold(w33)
    out_ref[dp, two:] = jnp.concatenate((w31, w32), axis=1)
    for copy in share(1):
        copy.start()
    for part in (0, 1):
        for copy in share(part):
            copy.wait()


class First:
    def __init__(self, part, acc, far, near, sem_far, sem_near, sem_send):
        self.part, self.level, self.acc, self.far, self.near = part, 0, acc, far, near
        self.size = far.shape[1] * BLK * 2 * BLK * 4
        self.sem_far, self.sem_near, self.sem_send = sem_far, sem_near, sem_send
        self.to = [neighbour(part, 1), neighbour(part, -1)]
        self.rows = pl.ds(part * BLK, BLK)

    def parity(self, slot):
        return (slot + slot // RING) % 2

    def visit(self, block, slot):
        return ((block, slot), (slot, block), (slot // RING, slot % RING))[self.part]

    def slot(self, visit):
        a, b = visit
        return (b, a, RING * a + b)[self.part]

    def block(self, visit):
        return (visit[0], visit[1], None)[self.part]

    def at(self, block, slot):
        return self.visit(block, slot) + (pl.ds(block, 1) if self.part == 2 else pl.ds(0, RING), self.rows)

    def whole(self, block):
        spot = [pl.ds(0, RING)] * 3
        spot[self.part] = pl.ds(block, 1)
        return self.acc.at[tuple(spot) + (self.rows,)]

    def far_copy(self, slot):
        return remote(
            self.acc.at[self.at(2, slot)], self.far.at[slot], self.sem_send.at[0], self.sem_far.at[slot], self.to[self.parity(slot)]
        )

    def near_copy(self, d, slot):
        return remote(
            self.acc.at[self.at((1, 3)[d], slot)], self.near.at[d, slot], self.sem_send.at[1 + d], self.sem_near.at[d, slot], self.to[d]
        )

    def relay(self, slot):
        self.acc[self.at((1, 3)[self.parity(slot)], slot)] += self.far[slot]

    def members(self, group):
        return ([group], list(range(RING)), [RING * group + b for b in range(RING)])[self.part]

    def settle(self, group):
        for slot in self.members(group):
            if self.part == 1:
                self.acc[slot, 0, group, self.rows] += self.near[0, slot, group] + self.near[1, slot, group]
            else:
                self.acc[self.at(0, slot)] += self.near[0, slot] + self.near[1, slot]

    def finish(self):
        for sem, block in enumerate((2, 1, 3)):
            whole = self.whole(block)
            remote(whole, whole, self.sem_send.at[sem], self.sem_far.at[0], self.to[0]).wait_send()


class Later:
    def __init__(self, part, level, acc, far, near, sem_far, sem_near, sem_send):
        self.part, self.level, self.acc, self.far, self.near = part, level, acc, far, near
        self.size = (1 if level == 2 else RING) * HALF * 2 * BLK * 4
        self.sem_far, self.sem_near, self.sem_send = sem_far, sem_near, sem_send
        self.axis = ORDERS[part][level]
        self.free = ORDERS[part][level + 1 :]
        self.to = [neighbour(self.axis, 1), neighbour(self.axis, -1)]

    def pick(self, block, group):
        spot = [pl.ds(0, 1)] * 3
        for axis in self.free:
            spot[axis] = pl.ds(0, RING) if group is None else pl.ds(group, 1)
        spot[self.axis] = pl.ds(block, 1)
        return tuple(spot)

    def rows(self, half):
        return (pl.ds(self.part * BLK + half * HALF, HALF),)

    def copy(self, src, dst, send, recv, d):
        return remote(self.acc.at[src], dst, self.sem_send.at[send, d], recv, self.to[d])

    def far_copy(self, d):
        return self.copy(self.pick(2, None) + self.rows(d), self.far.at[(d,) + self.pick(0, None)], 0, self.sem_far.at[d], d)

    def direct_copy(self, d):
        half = self.near.at[(d,) + self.pick(0, None) + (pl.ds((1 - d) * HALF, HALF),)]
        return self.copy(self.pick((1, 3)[d], None) + self.rows(1 - d), half, 1, self.sem_near.at[d, RING], d)

    def near_copy(self, d, group):
        half = self.near.at[(d,) + self.pick(0, group) + (pl.ds(d * HALF, HALF),)]
        return self.copy(self.pick((1, 3)[d], group) + self.rows(d), half, 2, self.sem_near.at[d, group or 0], d)

    def groups(self):
        return FAR_FIRST if self.free else (0,)

    def relay(self, d):
        self.acc[self.pick((1, 3)[d], None) + self.rows(d)] += self.far[(d,) + self.pick(0, None)]

    def settle(self, group):
        spot = self.pick(0, group)
        self.acc[spot + (pl.ds(self.part * BLK, BLK),)] += self.near[(0,) + spot] + self.near[(1,) + spot]

    def finish(self):
        for d in (0, 1):
            for copy in (self.far_copy(d), self.direct_copy(d), self.near_copy(d, None)):
                copy.wait_send()


class Last:
    def __init__(self, part, acc, near, sem_near, sem_send):
        self.part, self.level, self.acc, self.near, self.sem_near, self.sem_send = part, 2, acc, near, sem_near, sem_send
        self.axis = ORDERS[part][2]
        self.rows = pl.ds(part * BLK, BLK)
        self.size = BLK * 2 * BLK * 4

    def copy(self, block):
        spot = [0, 0, 0]
        spot[self.axis] = block
        return remote(
            self.acc.at[tuple(spot) + (self.rows,)],
            self.near.at[block - 1],
            self.sem_send.at[block - 1],
            self.sem_near.at[block - 1],
            neighbour(self.axis, block),
        )

    def settle(self):
        self.acc[0, 0, 0, self.rows] += self.near[0] + self.near[1] + self.near[2]

    def finish(self):
        for block in (1, 2, 3):
            self.copy(block).wait_send()


def factor_kernel(total, rows_ref, weights_ref, damp_ref, out_ref, acc, sent, got, mine, wide, columns, *rest):
    x, y, z, core = place()
    sem_in, sem_core, sem_share = rest[-3:]
    stages = [
        [First(part, acc, *rest[5 * part :][:5]) for part in range(3)],
        [Later(part, 1, acc, *rest[15 + 5 * part :][:5]) for part in range(3)],
        [Last(part, acc, *rest[30 + 3 * part :][:3]) for part in range(3)],
    ]
    span = RING * HD
    partner = {"head": lax.axis_index("head") // 2 * 2 + 1 - core}
    count = len(VISITS)
    trips = [(0, 0)]
    for i in range(count):
        trips += [(i + 1, 0)] * (i + 1 < count) + [(i, 1)]
    turn = {trip: v for v, trip in enumerate(trips)}

    def fetch(v):
        i, own = trips[v]
        to_x, to_y = (x + VISITS[i][0]) % RING, (y + VISITS[i][1]) % RING
        to_core = core if own else 1 - core
        first = ((to_x * 2 + to_y // 2) * 2 + to_core) * 8 + to_y % 2 * RING
        start = pl.multiple_of(first * HD, 2 * BLK)
        slot = v % AHEAD
        return pltpu.make_async_copy(rows_ref.at[:, pl.ds(start, span)], columns.at[slot], sem_in.at[slot])

    n_dp = out_ref.shape[0]
    peers = [{"dp": lax.rem(lax.axis_index("dp") + o, n_dp)} for o in range(1, n_dp)]
    met = greet([partner] + [to for stage in stages[0] for to in stage.to] + [neighbour(axis, 2) for axis in range(3)] + peers)
    for v in range(AHEAD):
        fetch(v).start()
    for k in range(wide.shape[0] // (2 * BLK)):
        power = weights_ref[pl.ds(2 * BLK * k, 2 * BLK)].reshape(1, 2 * BLK)
        weight = jnp.where(power % 2 == 1, 2.0, 1.0) * jnp.where(power >= 2, 4.0, 1.0)
        block = jnp.broadcast_to(weight, (2 * BLK, 2 * BLK)).T.astype(wide.dtype)
        for j in range(3):
            wide[2 * BLK * k : 2 * BLK * (k + 1), 2 * BLK * j : 2 * BLK * (j + 1)] = block

    def multiply(v, out):
        for i in range(RING // 2):
            even = (2 * i + RING - z) % RING
            store_pair(columns[v % AHEAD, :, 2 * i * HD : 2 * (i + 1) * HD], wide[...], out, even, (even + 1) % RING)

    def exchange(i):
        return remote(sent.at[i], got.at[i], sem_core.at[0, i], sem_core.at[1, i], partner)

    def add(i):
        a, b = VISITS[i]
        acc[a, b] = mine[i % 2] + got[i]

    events = []
    links = {}

    def message(copy, stage, d, rank, key, pieces=1):
        links[key] = (copy, (ORDERS[stage.part][stage.level], d), stage.size // pieces, rank)
        return key

    def plan(name, needs, arrivals, work, sends):
        events.append((name, needs, arrivals, work, sends))

    for i, spot in enumerate(VISITS):
        sends = []
        for s in stages[0]:
            slot = s.slot(spot)
            if s.block(spot) in (2, None):
                sends.append(message(s.far_copy(slot), s, s.parity(slot), 0, (s, "far", slot)))
            side = 1 - s.parity(slot)
            if s.block(spot) in ((1, 3)[side], None):
                sends.append(message(s.near_copy(side, slot), s, side, 2, (s, "near", side, slot)))
        plan(spot, [], [i], functools.partial(add, i), sends)
    for s, t, u in zip(*stages):
        for slot in range(s.near.shape[1]):
            d = s.parity(slot)
            send = message(s.near_copy(d, slot), s, d, 1, (s, "near", d, slot))
            plan((s, "relay", slot), [s.visit((1, 3)[d], slot)], [(s, "far", slot)], functools.partial(s.relay, slot), [send])
        for group in FAR_FIRST:
            slots = s.members(group)
            arrivals = [(s, "near", d, slot) for d in (0, 1) for slot in slots]
            sends = []
            if group == 2:
                sends = [message(t.far_copy(d), t, d, 0, (t, "far", d)) for d in (0, 1)]
            elif group:
                sends = [message(t.direct_copy(group // 2), t, group // 2, 2, (t, "direct", group // 2))]
            plan((s, group), [s.visit(0, slot) for slot in slots], arrivals, functools.partial(s.settle, group), sends)
        for d in (0, 1):
            sends = [message(t.near_copy(d, g), t, d, 1, (t, "near", d, g), RING) for g in FAR_FIRST]
            plan((t, "relay", d), [(s, (1, 3)[d])], [(t, "far", d)], functools.partial(t.relay, d), sends)
        for g in FAR_FIRST:
            arrivals = [(t, "near", d, g) for d in (0, 1)] + [(t, "direct", d) for d in (0, 1)]
            sends = [message(u.copy(g), u, g // 3, 0, (u, g))] if g else []
            plan((t, g), [(s, 0)], arrivals, functools.partial(t.settle, g), sends)
        plan((u, 0), [(t, 0)], [(u, block) for block in (1, 2, 3)], u.settle, [])

    done, waited, due, free = set(), set(), {}, {}
    pending = list(events)
    clock = 0.0
    r = -1
    while pending:
        now = [turn[trip] for trip in ((r + 1, 0), (r, 1)) if trip in turn]
        ready = []
        for event in list(pending):
            name, needs, arrivals, _, _ = event
            if isinstance(arrivals[0], int):
                fit = arrivals[0] == r - 1
            else:
                fit = all(n in done for n in needs) and all(due.get(m, 1e9) <= clock for m in arrivals)
            if fit:
                ready.append(event)
                pending.remove(event)
                done.add(name)
        for v in now:
            fetch(v).wait()
        for _, _, arrivals, _, _ in ready:
            for m in arrivals:
                if m not in waited:
                    waited.add(m)
                    (exchange(m) if isinstance(m, int) else links[m][0]).wait_recv()
        for v in now:
            i, own = trips[v]
            multiply(v, mine.at[i % 2] if own else sent.at[i])
        for _, _, _, work, _ in ready:
            work()
        if r == -1:
            met()
        if r + 1 < count:
            exchange(r + 1).start()
        for v in now:
            if v + AHEAD < len(trips):
                fetch(v + AHEAD).start()
        clock += VISIT_US if r <= count else TAIL_US
        for m in sorted((m for event in ready for m in event[4]), key=lambda m: links[m][3]):
            copy, link, size, _ = links[m]
            copy.start()
            free[link] = max(free.get(link, 0.0), clock) + size / LINK_RATE + 0.08
            due[m] = free[link] + HOP_US
        r += 1
    whiten(acc[0, 0, 0], damp_ref, total, out_ref, sem_share)
    for i in range(count):
        exchange(i).wait_send()
    for level in stages:
        for stage in level:
            stage.finish()


def factors(projected, weights, damp_exp, total, n_dp):
    tokens, width = projected.shape
    rows, lanes = HD, 2 * BLK
    f32 = jnp.float32
    rings = []
    for level in range(3):
        for part in range(3):
            if level:
                free = ORDERS[part][level + 1 :]
                far = (2,) + tuple(RING if a in free else 1 for a in range(3)) + (HALF, lanes)
                near = far[:-2] + (BLK, lanes)
                sems = (2,), (2, RING + 1), (3, 2)
                if level == 2:
                    rings += [pltpu.VMEM((3, BLK, lanes), f32), *map(pltpu.SemaphoreType.DMA, ((3,), (3,)))]
                    continue
            else:
                slots, each = ((RING, RING), (RING, RING), (RING * RING, 1))[part]
                far = (slots, each, BLK, lanes)
                near = (2,) + far
                sems = (slots,), (2, slots), (3,)
            rings += [pltpu.VMEM(far, f32), pltpu.VMEM(near, f32), *map(pltpu.SemaphoreType.DMA, sems)]
    return pl.pallas_call(
        functools.partial(factor_kernel, total),
        in_specs=[
            pl.BlockSpec(memory_space=pl.ANY),
            pl.BlockSpec(memory_space=pltpu.VMEM),
            pl.BlockSpec(memory_space=pltpu.SMEM),
        ],
        out_specs=pl.BlockSpec(memory_space=pltpu.VMEM),
        out_shape=jax.ShapeDtypeStruct((n_dp, rows, lanes), f32),
        scratch_shapes=[
            pltpu.VMEM((RING, RING, RING, rows, lanes), f32),
            pltpu.VMEM((len(VISITS), RING, rows, lanes), f32),
            pltpu.VMEM((len(VISITS), RING, rows, lanes), f32),
            pltpu.VMEM((2, RING, rows, lanes), f32),
            pltpu.VMEM((tokens, 2 * HD), projected.dtype),
            pltpu.VMEM((AHEAD, tokens, RING * HD), projected.dtype),
            *rings,
            pltpu.SemaphoreType.DMA((AHEAD,)),
            pltpu.SemaphoreType.DMA((2, len(VISITS))),
            pltpu.SemaphoreType.DMA((2, 2, n_dp - 1)),
        ],
        compiler_params=pltpu.CompilerParams(collective_id=0, has_side_effects=True, vmem_limit_bytes=60 << 20),
    )(projected, weights, damp_exp)


def unpack_kernel(packed_ref, out_ref, whole, sems):
    two, early = 2 * BLK, HD // 2
    copies = []
    for m in range(packed_ref.shape[0]):
        whole[m, :BLK, :BLK] = packed_ref[m, :BLK, :BLK]
        whole[m, :BLK, BLK:] = jnp.zeros((BLK, two), jnp.float32)
        side = packed_ref[m, BLK:early]
        below = jnp.concatenate((side[:, :BLK], side[:, BLK:]), axis=0)
        right = lax.broadcasted_iota(jnp.int32, (BLK, two), 1) >= BLK
        whole[m, BLK:two, :two] = jnp.where(right, packed_ref[m, :BLK], jnp.concatenate((below, below), axis=1))
        whole[m, BLK:two, two:] = jnp.zeros((BLK, BLK), jnp.float32)
        whole[m, two:, :two] = packed_ref[m, two:]
        last = packed_ref[m, early:two]
        whole[m, two:, two:] = jnp.concatenate((last[:, :BLK], last[:, BLK:]), axis=0)
        copy = pltpu.make_async_copy(whole.at[m], out_ref.at[m], sems.at[m])
        copy.start()
        copies.append(copy)
    for copy in copies:
        copy.wait()


def unpack(packed):
    shape = (packed.shape[0], HD, HD)
    return pl.pallas_call(
        unpack_kernel,
        in_specs=[pl.BlockSpec(memory_space=pltpu.VMEM)],
        out_specs=pl.BlockSpec(memory_space=pl.ANY),
        out_shape=jax.ShapeDtypeStruct(shape, jnp.float32),
        scratch_shapes=[pltpu.VMEM(shape, jnp.float32), pltpu.SemaphoreType.DMA(shape[:1])],
    )(packed)


def on_device(projected, weight_exp, damp_exp):
    n_dp = lax.axis_size("dp")
    total = projected.shape[0] * lax.axis_size("head") * n_dp
    return unpack(factors(projected, weight_exp, damp_exp, float(total), n_dp))


def solution(mesh):
    return jax.shard_map(
        on_device,
        mesh=mesh,
        in_specs=(P(("dp", "head"), None), P(("dp", "head")), P()),
        out_specs=P("head", None, None),
        check_vma=False,
    )
```
